256 devices in a mesh: patch: 32 (over y, z_hi, core), chan: 8 (over z_lo, x).
Axes of the slice: x: 4, y: 4, z: 8 (z_hi: 4, z_lo: 2; z = z_hi * 2 + z_lo), core: 2. Of those that a mesh axis runs over, the one named last changes fastest.
Arguments:
- tokens: bfloat16 [1, 16384, 1280], P(None, 'patch'), may hold values from -12 to 12
- stale_k: bfloat16 [1, 16384, 1024], P(None, 'patch', 'chan'), may hold values from -64 to 64
- stale_v: bfloat16 [1, 16384, 1024], P(None, 'patch', 'chan'), may hold values from -6 to 6
- w_query: bfloat16 [1280, 1024], P(None, 'chan'), may hold values from -0.15625 to 0.15625
- w_key: bfloat16 [1280, 1024], P(None, 'chan'), may hold values from -0.4375 to 0.4375
- w_value: bfloat16 [1280, 1024], P(None, 'chan'), may hold values from -0.15625 to 0.15625
- w_out: bfloat16 [1024, 1280], P('chan'), may hold values from -0.1875 to 0.1875
- ff_value: bfloat16 [1280, 5120], P(None, 'chan'), may hold values from -0.15625 to 0.15625
- ff_gate: bfloat16 [1280, 5120], P(None, 'chan'), may hold values from -0.15625 to 0.15625
- ff_down: bfloat16 [5120, 1280], P('chan'), may hold values from -0.078125 to 0.078125
Outputs:
- layer_out: bfloat16 [1, 16384, 1280], P(None, 'patch', 'chan')
The draws below stay inside these ranges and needn't reach their ends.
All inputs are finite; a program needn't handle non-finite values.
Results may differ from the reference program's by a relative error of at most 0.0095.
Values may be sent and summed in bfloat16 or wider, within the bound.
A program may use at most 64 MiB of HBM per device.

```python
import math
import jax
import jax.numpy as jnp
from jax import lax

D = 1280
HEADS = 16
HD = 64
FF = 5120
TOK_DEV = 512
BATCH = 1
TOKENS = 16384
N_PATCH = 32


def draw_tokens(key, part):
    key_base, key_cols = jax.random.split(jax.random.fold_in(key, 11), 2)
    shape = (BATCH, TOKENS, D)
    columns = jnp.exp(jax.random.uniform(key_cols, (D,), jnp.float32, math.log(0.3), math.log(3.0)))
    base = jax.random.normal(key_base, shape, jnp.float32) * columns
    return jnp.clip(base, -12.0, 12.0).astype(jnp.bfloat16)


def draw_stale_k(key, part):
    key_base = jax.random.fold_in(jax.random.fold_in(key, 23), 0)
    shape = (BATCH, TOKENS, HEADS * HD)
    base = jnp.clip(2.5 * jax.random.normal(key_base, shape, jnp.float32), -10.0, 10.0)
    return base.astype(jnp.bfloat16)


def block_scale(stream_key, shape, pieces, least, largest):
    level, own = 1.0, jax.random.fold_in(stream_key, 6)
    for axis_at, blocks in pieces:
        draws = jnp.exp(jax.random.uniform(jax.random.fold_in(own, axis_at), (blocks,), jnp.float32, least / len(pieces), largest / len(pieces)))
        level = level * jnp.repeat(draws, shape[axis_at] // blocks).reshape([-1 if axis == axis_at else 1 for axis in range(len(shape))])
    return level


def gaussian(rng, shape, scale, limit, cuts=(), held_as=jnp.bfloat16):
    values = jax.random.normal(rng, shape, jnp.float32) * scale
    if len(cuts) > 0:
        values = block_scale(rng, shape, cuts, -0.22, 0.18) * values
    return jnp.clip(values, min=-limit, max=limit).astype(held_as)


def setup_inputs(seed: int = 0) -> dict:
    key_list = jax.random.split(jax.random.key(seed), 11)
    tokens = draw_tokens(jax.random.fold_in(key_list[10], 71), 0)
    stale_k = draw_stale_k(jax.random.fold_in(key_list[10], 71), 0)
    stale_v = gaussian(key_list[2], (BATCH, TOKENS, HEADS * HD), 1.0, 6.0, ((1, 32), (2, 8)))
    w_query = gaussian(key_list[3], (D, HEADS * HD), D ** -0.5, 0.15625, ((1, 8),))
    w_key = gaussian(key_list[4], (D, HEADS * HD), (D // 6) ** -0.5, 0.4375, ((1, 8),))
    w_value = gaussian(key_list[5], (D, HEADS * HD), D ** -0.5, 0.15625, ((1, 8),))
    w_out = gaussian(key_list[6], (HEADS * HD, D), (HEADS * HD) ** -0.5, 0.1875, ((0, 8),))
    ff_value = gaussian(key_list[7], (D, FF), D ** -0.5, 0.15625, ((1, 8),))
    ff_gate = gaussian(key_list[8], (D, FF), D ** -0.5, 0.15625, ((1, 8),))
    ff_down = gaussian(key_list[9], (FF, D), FF ** -0.5, 0.078125, ((0, 8),))
    return {"tokens": tokens, "stale_k": stale_k, "stale_v": stale_v, "w_query": w_query, "w_key": w_key, "w_value": w_value, "w_out": w_out, "ff_value": ff_value, "ff_gate": ff_gate, "ff_down": ff_down}


def layer_norm(values):
    mean = lax.optimization_barrier(jnp.mean(values, axis=-1, keepdims=True))
    centered = values - mean
    var = lax.optimization_barrier(jnp.mean(centered * centered, axis=-1, keepdims=True))
    return centered * lax.rsqrt(var + 1e-05)

def to_wide(values):
    return lax.optimization_barrier(values).astype(jnp.float32)

def project(inputs, weight):
    return jnp.einsum('btd,de->bte', inputs.astype(jnp.float32), weight.astype(jnp.float32))

def reference(tokens, stale_k, stale_v, w_query, w_key, w_value, w_out, ff_value, ff_gate, ff_down):
    normed = layer_norm(tokens.astype(jnp.float32)).astype(jnp.bfloat16)
    queries = project(to_wide(normed), w_query).astype(jnp.bfloat16)
    key_fresh = project(to_wide(normed), w_key).astype(jnp.bfloat16)
    value_fresh = project(to_wide(normed), w_value).astype(jnp.bfloat16)
    shape_four = (BATCH, TOKENS, HEADS, HD)
    queries = queries.reshape(shape_four)
    key_fresh = key_fresh.reshape(shape_four)
    value_fresh = value_fresh.reshape(shape_four)
    stale_keys = stale_k.reshape(shape_four)
    stale_values = stale_v.reshape(shape_four)
    score_scale = 1.0 / HD ** 0.5

    def per_patch(patch_id):
        first_row = (patch_id * TOK_DEV).astype(jnp.int32)
        query_rows = lax.dynamic_slice_in_dim(queries, first_row, TOK_DEV, 1)
        fresh_keys = lax.dynamic_slice_in_dim(key_fresh, first_row, TOK_DEV, 1)
        fresh_values = lax.dynamic_slice_in_dim(value_fresh, first_row, TOK_DEV, 1)
        key_rows = lax.dynamic_update_slice_in_dim(stale_keys, fresh_keys, first_row, 1)
        value_rows = lax.dynamic_update_slice_in_dim(stale_values, fresh_values, first_row, 1)
        scores = jnp.einsum('bqhd,bkhd->bhqk', to_wide(query_rows), to_wide(key_rows)) * score_scale
        running_max = lax.optimization_barrier(jnp.max(scores, axis=-1, keepdims=True))
        weights = jnp.exp(scores - running_max)
        totals = lax.optimization_barrier(jnp.sum(weights, axis=-1))
        rounded = to_wide(weights.astype(jnp.bfloat16))
        accum = jnp.einsum('bhqk,bkhd->bhqd', rounded, to_wide(value_rows))
        result = accum / totals[..., None]
        return jnp.transpose(result, (0, 2, 1, 3)).reshape(BATCH, TOK_DEV, HEADS * HD)
    patches = lax.map(per_patch, jnp.arange(N_PATCH, dtype=jnp.int32))
    attended = jnp.transpose(patches, (1, 0, 2, 3)).reshape(BATCH, TOKENS, HEADS * HD).astype(jnp.bfloat16)
    resid = tokens.astype(jnp.float32) + project(to_wide(attended), w_out)
    normed_two = layer_norm(resid).astype(jnp.bfloat16)
    ff_val = project(to_wide(normed_two), ff_value)
    gate_out = project(to_wide(normed_two), ff_gate)
    gated = (ff_val * jax.nn.gelu(gate_out, approximate=False)).astype(jnp.bfloat16)
    layer_out = resid + project(to_wide(gated), ff_down)
    return layer_out.astype(jnp.bfloat16)
```

```python
import functools
import math

import jax
import jax.numpy as jnp
from jax import lax
from jax.experimental import pallas as pl
from jax.experimental.pallas import tpu as pltpu
from jax.sharding import PartitionSpec as P

HD = 64
MESH = pl.DeviceIdType.MESH
F32 = jnp.float32
BF16 = jnp.bfloat16
LOW = -1e30
SCALE = math.log2(math.e) / math.sqrt(HD)


def normalize(values):
    mean = jnp.mean(values, axis=-1, keepdims=True)
    centered = values - mean
    var = jnp.mean(centered * centered, axis=-1, keepdims=True)
    return centered * lax.rsqrt(var + 1e-05)


def attention_kernel(
    tok, k_in, v_in, w_q, w_k, w_v, out,
    normed, kvb, kvo, qb, qo, kk, qq, s_a, s_b, b_a, b_b,
    top, total, acc, stat_out, o_out, o_in, stat_in, fin,
    kv_send, kv_recv, q_send, q_recv, o_send, o_recv, t_send, t_recv,
):
    p, c = lax.axis_index("patch"), lax.axis_index("chan")
    s = lax.rem(p, 2)
    z = lax.rem(lax.div(p, 2), 4)
    y = lax.div(p, 8)
    t = 1 - s
    y_up, y_down = lax.rem(y + 1, 4), lax.rem(y + 3, 4)
    z_up, z_down = lax.rem(z + 1, 4), lax.rem(z + 3, 4)

    def dev(y, z, s):
        return ((y * 4 + z) * 2 + s, c)

    partner = dev(y, z, t)
    rows = tok.shape[0]

    barrier = pltpu.get_barrier_semaphore()
    peers = [partner]
    for core in (s, t):
        peers += [dev(y_up, z, core), dev(y_down, z, core)]
        peers += [dev(y, z_up, core), dev(y, z_down, core)]
    for peer in peers:
        pl.semaphore_signal(barrier, inc=1, device_id=peer, device_id_type=MESH)
    pl.semaphore_wait(barrier, len(peers))

    def split_heads(values):
        first, second = values[:HD], values[HD:]
        mine = jnp.where(s == 0, first, second)
        other = jnp.where(s == 0, second, first)
        return mine, other

    def copy(src, dst, send, recv, peer):
        return pltpu.make_async_remote_copy(
            src_ref=src, dst_ref=dst, send_sem=send, recv_sem=recv,
            device_id=peer, device_id_type=MESH,
        )

    for j, ref in enumerate((k_in, v_in)):
        mine, other = split_heads(ref[...].T)
        kvb[0, j] = mine
        kvo[0, j] = other
    kv = {
        2: copy(kvb.at[0], kvb.at[2], kv_send.at[2], kv_recv.at[2], dev(y_up, z, s)),
        3: copy(kvo.at[0], kvb.at[3], kv_send.at[3], kv_recv.at[3], dev(y_down, z, t)),
        1: copy(kvo.at[0], kvb.at[1], kv_send.at[1], kv_recv.at[1], partner),
        4: copy(kvo.at[0], kvb.at[4], kv_send.at[4], kv_recv.at[4], dev(y_up, z, t)),
        5: copy(kvb.at[0], kvb.at[5], kv_send.at[5], kv_recv.at[5], dev(y_down, z, s)),
        6: copy(kvb.at[2], kvb.at[6], kv_send.at[6], kv_recv.at[6], dev(y_up, z, s)),
        7: copy(kvb.at[3], kvb.at[7], kv_send.at[7], kv_recv.at[7], dev(y_down, z, s)),
        9: copy(kvo.at[1], kvb.at[9], kv_send.at[9], kv_recv.at[9], partner),
    }
    for j in (2, 3, 1, 4, 5):
        kv[j].start()

    step = 128

    def norm_rows(i, _):
        at = pl.ds(pl.multiple_of(i * step, step), step)
        normed[at, :] = normalize(tok[at, :].astype(F32)).astype(BF16)
        return 0

    lax.fori_loop(0, rows // step, norm_rows, 0)

    def project(w):
        return jnp.dot(normed[...], w[...], preferred_element_type=F32).astype(BF16)

    mine, other = split_heads(project(w_q).T)
    qb[0] = mine
    qo[...] = other
    q = {
        2: copy(qb.at[0], qb.at[2], q_send.at[2], q_recv.at[2], dev(y, z_up, s)),
        3: copy(qo, qb.at[3], q_send.at[3], q_recv.at[3], dev(y, z_down, t)),
        4: copy(qo, qb.at[4], q_send.at[4], q_recv.at[4], dev(y, z_up, t)),
        5: copy(qb.at[0], qb.at[5], q_send.at[5], q_recv.at[5], dev(y, z_down, s)),
        1: copy(qo, qb.at[1], q_send.at[1], q_recv.at[1], partner),
        6: copy(qb.at[2], qb.at[6], q_send.at[6], q_recv.at[6], dev(y, z_up, s)),
        7: copy(qb.at[3], qb.at[7], q_send.at[7], q_recv.at[7], dev(y, z_down, s)),
    }
    for j in (2, 3, 4, 5, 1):
        q[j].start()
    for j, w in enumerate((w_k, w_v)):
        mine, other = split_heads(project(w).T)
        kvb[8, j] = mine
        kvo[1, j] = other
    kv[9].start()

    top[...] = jnp.full(top.shape, LOW, F32)
    total[...] = jnp.zeros(total.shape, F32)
    acc[...] = jnp.zeros(acc.shape, F32)

    def prepare_keys(u):
        key = kvb[u, 0]
        kk[u] = jnp.concatenate([key, key], axis=0).T

    def prepare_queries(f):
        scaled = qb[f].astype(F32) * SCALE
        high = scaled.astype(BF16)
        low = (scaled - high.astype(F32)).astype(BF16)
        qq[f] = jnp.concatenate([high, low], axis=0)

    def score(f, u, s_ref, b_ref):
        values = jnp.dot(kk[u], qq[f], preferred_element_type=F32)
        s_ref[...] = values
        b_ref[...] = jnp.max(values, axis=0, keepdims=True)

    def absorb(f, u, s_ref, b_ref):
        old = top[f]
        new = jnp.maximum(old, b_ref[...])
        rescale = jnp.exp2(old - new)
        weights = jnp.exp2(s_ref[...] - new)
        total[f] = total[f] * rescale + jnp.sum(weights, axis=0, keepdims=True)
        acc[f] = acc[f] * rescale + jnp.dot(
            kvb[u, 1], weights.astype(BF16), preferred_element_type=F32
        )
        top[f] = new

    def attend(count, pair):
        score(*pair(0), s_a, b_a)

        def two(i, _):
            first, second = pair(2 * i), pair(2 * i + 1)
            third = pair(jnp.minimum(2 * i + 2, count - 1))
            score(*second, s_b, b_b)
            absorb(*first, s_a, b_a)
            score(*third, s_a, b_a)
            absorb(*second, s_b, b_b)
            return 0

        lax.fori_loop(0, count // 2, two, 0)

    def block(f0, nf, u0, nu):
        attend(nf * nu, lambda i: (f0 + lax.div(i, nu), u0 + lax.rem(i, nu)))

    def own_pair(i):
        f, b = lax.div(i, 2), lax.rem(i, 2)
        return f, b + 8 * (1 - f - b + 2 * f * b)

    prepare_keys(0)
    prepare_keys(8)
    prepare_queries(0)
    kv[1].wait_recv()
    prepare_keys(1)
    q[1].wait_recv()
    prepare_queries(1)
    kv[9].wait_recv()
    prepare_keys(9)
    attend(4, lambda i: own_pair(jnp.int32(i)))

    for j in (2, 3):
        kv[j].wait_recv()
        kv[j + 4].start()
        prepare_keys(j)
    block(0, 2, 2, 2)

    for j in (2, 3):
        q[j].wait_recv()
        q[j + 4].start()
        prepare_queries(j)
    for j in (4, 5):
        kv[j].wait_recv()
        prepare_keys(j)
    block(2, 2, 0, 6)

    for j in (4, 5):
        q[j].wait_recv()
        prepare_queries(j)
    block(4, 2, 0, 6)

    for j in (6, 7):
        kv[j].wait_recv()
        prepare_keys(j)
        q[j].wait_recv()
        prepare_queries(j)
    block(6, 2, 0, 8)

    targets = {
        6: (dev(y, z_up, s), 5),
        7: (dev(y, z_down, s), 6),
        2: (dev(y, z_down, s), 1),
        3: (dev(y, z_up, t), 2),
        4: (dev(y, z_down, t), 3),
        5: (dev(y, z_up, s), 4),
        1: (partner, 0),
    }
    back = {}
    for f, (peer, slot) in targets.items():
        back[f] = (
            copy(o_out.at[f], o_in.at[slot], o_send.at[f], o_recv.at[slot], peer),
            copy(stat_out.at[f], stat_in.at[slot], t_send.at[f], t_recv.at[slot], peer),
        )

    def give(f):
        o_out[f] = acc[f].astype(BF16)
        stat_out[f, 0:1] = top[f]
        stat_out[f, 1:2] = total[f]
        for part in back[f]:
            part.start()

    def arrived(f):
        for part in back[f]:
            part.wait_recv()

    def merge(one, other):
        new = jnp.maximum(one[0], other[0])
        left, right = jnp.exp2(one[0] - new), jnp.exp2(other[0] - new)
        return (
            new,
            one[1] * left + other[1] * right,
            one[2] * left + other[2] * right,
        )

    def received(slot):
        return (
            stat_in[slot, 0:1], stat_in[slot, 1:2], o_in[slot].astype(F32),
        )

    def local(f):
        return top[f], total[f], acc[f]

    give(6)
    give(7)
    block(2, 4, 6, 2)
    give(2)
    give(3)
    arrived(6)
    arrived(7)
    for f, slot in ((5, 5), (4, 6)):
        top[f], total[f], acc[f] = merge(local(f), received(slot))
        give(f)
    block(1, 1, 4, 4)
    give(1)
    block(0, 1, 4, 4)

    for f in (1, 2, 3, 4, 5):
        arrived(f)
    _, sums, values = merge(merge(local(0), received(1)), received(4))
    fin[s] = values / sums
    _, sums, values = merge(merge(received(0), received(2)), received(3))
    fin[t] = values / sums
    out[...] = jnp.concatenate([fin[0], fin[1]], axis=0).T.astype(BF16)

    for j in (1, 2, 3, 4, 5, 6, 7, 9):
        kv[j].wait_send()
    for j in (1, 2, 3, 4, 5, 6, 7):
        q[j].wait_send()
        for part in back[j]:
            part.wait_send()


def attention(tokens, stale_k, stale_v, w_query, w_key, w_value):
    rows, width = tokens.shape
    vmem = pl.BlockSpec(memory_space=pltpu.VMEM)
    dma = pltpu.SemaphoreType.DMA
    return pl.pallas_call(
        attention_kernel,
        out_shape=jax.ShapeDtypeStruct((rows, 2 * HD), BF16),
        in_specs=[vmem] * 6,
        out_specs=vmem,
        scratch_shapes=[
            pltpu.VMEM((rows, width), BF16),
            pltpu.VMEM((10, 2, HD, rows), BF16),
            pltpu.VMEM((2, 2, HD, rows), BF16),
            pltpu.VMEM((8, HD, rows), BF16),
            pltpu.VMEM((HD, rows), BF16),
            pltpu.VMEM((10, rows, 2 * HD), BF16),
            pltpu.VMEM((8, 2 * HD, rows), BF16),
            pltpu.VMEM((rows, rows), F32),
            pltpu.VMEM((rows, rows), F32),
            pltpu.VMEM((1, rows), F32),
            pltpu.VMEM((1, rows), F32),
            pltpu.VMEM((8, 1, rows), F32),
            pltpu.VMEM((8, 1, rows), F32),
            pltpu.VMEM((8, HD, rows), F32),
            pltpu.VMEM((8, 2, rows), F32),
            pltpu.VMEM((8, HD, rows), BF16),
            pltpu.VMEM((7, HD, rows), BF16),
            pltpu.VMEM((7, 2, rows), F32),
            pltpu.VMEM((2, HD, rows), F32),
            dma((10,)), dma((10,)), dma((8,)), dma((8,)),
            dma((8,)), dma((7,)), dma((8,)), dma((7,)),
        ],
        compiler_params=pltpu.CompilerParams(collective_id=0, has_side_effects=True),
    )(tokens, stale_k, stale_v, w_query, w_key, w_value)


def split_up(shard, dim, devices):
    before, after = (shard.shape[:dim], shard.shape[dim + 1 :])
    return jnp.moveaxis(shard.reshape(*before, devices, -1, *after), dim, 0)


def sent_and_summed(shard, axis, dim):
    devices = lax.axis_size(axis)
    pieces = lax.all_to_all(split_up(shard, dim, devices), axis, 0, 0, tiled=True)
    return jnp.sum(pieces.astype(jnp.float32), axis=0)


def in_order(pieces, dim):
    lengths = list(pieces.shape[1:])
    lengths[dim] *= pieces.shape[0]
    return jnp.moveaxis(pieces, 0, dim).reshape(lengths)


def from_everyone(shard, axis):
    copies = jnp.broadcast_to(shard, (lax.axis_size(axis), *shard.shape))
    return lax.all_to_all(copies, axis, split_axis=0, concat_axis=0, tiled=True)


def collect(shard, axis, dim):
    return in_order(from_everyone(shard, axis), dim)


def project(inputs, weight):
    return jnp.einsum("btd,de->bte", inputs, weight, preferred_element_type=jnp.float32)


def per_device(
    tokens, stale_k, stale_v, w_query, w_key, w_value, w_out, ff_value, ff_gate, ff_down
):
    batch_size, row_count, width = tokens.shape
    attended = attention(
        tokens[0], stale_k[0], stale_v[0], w_query, w_key, w_value
    )[None]
    partial_value = project(attended, w_out)
    chan_id = lax.axis_index("chan")
    share_width = width // lax.axis_size("chan")
    attn_part = sent_and_summed(partial_value.astype(jnp.bfloat16), "chan", 2)
    resid_share = (
        lax.dynamic_slice_in_dim(tokens, chan_id * share_width, share_width, 2).astype(jnp.float32)
        + attn_part
    )
    resid = collect(resid_share.astype(jnp.bfloat16), "chan", 2).astype(resid_share.dtype)
    normed_two = normalize(resid).astype(jnp.bfloat16)
    ff_val = project(normed_two, ff_value)
    gate_out = project(normed_two, ff_gate)
    gated = (ff_val * jax.nn.gelu(gate_out, approximate=False)).astype(jnp.bfloat16)
    down_out = project(gated, ff_down)
    ffn_part = sent_and_summed(down_out.astype(jnp.bfloat16), "chan", 2)
    return (resid_share + ffn_part).astype(jnp.bfloat16)


def solution(mesh):
    return jax.shard_map(
        per_device,
        mesh=mesh,
        in_specs=(
            P(None, "patch", None),
            P(None, "patch", "chan"),
            P(None, "patch", "chan"),
            P(None, "chan"),
            P(None, "chan"),
            P(None, "chan"),
            P("chan", None),
            P(None, "chan"),
            P(None, "chan"),
            P("chan", None),
        ),
        out_specs=P(None, "patch", "chan"),
        check_vma=False,
    )
```

```python
import functools
import math

import jax
import jax.numpy as jnp
from jax import lax
from jax.experimental import pallas as pl
from jax.experimental.pallas import tpu as pltpu
from jax.sharding import PartitionSpec as P

HD = 64
MESH = pl.DeviceIdType.MESH
F32 = jnp.float32
BF16 = jnp.bfloat16
LOW = -1e30
SCALE = math.log2(math.e) / math.sqrt(HD)


def normalize(values):
    mean = jnp.mean(values, axis=-1, keepdims=True)
    centered = values - mean
    var = jnp.mean(centered * centered, axis=-1, keepdims=True)
    return centered * lax.rsqrt(var + 1e-05)


def block_kernel(
    tok_hbm, k_hbm, v_hbm, wq_hbm, wk_hbm, wv_hbm, wo_hbm, fv_hbm, fg_hbm, fd_hbm, out,
    tok, k_in, v_in, w_q, w_k, w_v, w_o, f_v, f_g, f_d,
    normed, kvb, kvo, qb, qo, kk, qq, s_a, s_b, b_a, b_b,
    top, total, acc, stat_out, o_out, o_in, stat_in, fin,
    att, resid, turned, down, pieces,
    load, kv_send, kv_recv, q_send, q_recv, o_send, o_recv, t_send, t_recv,
    w_send, w_recv, wx_send, wx_recv, a_send, a_recv, r_send, r_recv,
):
    p, c = lax.axis_index("patch"), lax.axis_index("chan")
    s = lax.rem(p, 2)
    z = lax.rem(lax.div(p, 2), 4)
    y = lax.div(p, 8)
    t = 1 - s
    y_up, y_down = lax.rem(y + 1, 4), lax.rem(y + 3, 4)
    z_up, z_down = lax.rem(z + 1, 4), lax.rem(z + 3, 4)
    across, along = lax.div(c, 4), lax.rem(c, 4)
    rows = tok.shape[0]
    half = rows // 2
    share = out.shape[1]

    def dev(y, z, s):
        return ((y * 4 + z) * 2 + s, c)

    partner = dev(y, z, t)

    def chan_of(j):
        return lax.rem(across + j // 4, 2) * 4 + lax.rem(along + j % 4, 4)

    loads = [
        pltpu.make_async_copy(src, dst, load.at[i])
        for i, (src, dst) in enumerate(
            (
                (k_hbm, k_in), (v_hbm, v_in), (tok_hbm, tok), (wq_hbm, w_q),
                (wk_hbm, w_k), (wv_hbm, w_v), (wo_hbm, w_o.at[0]), (fv_hbm, f_v),
                (fg_hbm, f_g), (fd_hbm, f_d),
            )
        )
    ]
    for part in loads:
        part.start()

    barrier = pltpu.get_barrier_semaphore()
    peers = [partner]
    for core in (s, t):
        peers += [dev(y_up, z, core), dev(y_down, z, core)]
        peers += [dev(y, z_up, core), dev(y, z_down, core)]
    peers += [(p, chan_of(j)) for j in range(1, 8)]
    for peer in peers:
        pl.semaphore_signal(barrier, inc=1, device_id=peer, device_id_type=MESH)
    pl.semaphore_wait(barrier, len(peers))

    def split_heads(values):
        first, second = values[:HD], values[HD:]
        mine = jnp.where(s == 0, first, second)
        other = jnp.where(s == 0, second, first)
        return mine, other

    def copy(src, dst, send, recv, peer):
        return pltpu.make_async_remote_copy(
            src_ref=src, dst_ref=dst, send_sem=send, recv_sem=recv,
            device_id=peer, device_id_type=MESH,
        )

    for j, ref in enumerate((k_in, v_in)):
        loads[j].wait()
        mine, other = split_heads(ref[...].T)
        kvb[0, j] = mine
        kvo[0, j] = other
    kv = {
        2: copy(kvb.at[0], kvb.at[2], kv_send.at[2], kv_recv.at[2], dev(y_up, z, s)),
        3: copy(kvo.at[0], kvb.at[3], kv_send.at[3], kv_recv.at[3], dev(y_down, z, t)),
        1: copy(kvo.at[0], kvb.at[1], kv_send.at[1], kv_recv.at[1], partner),
        4: copy(kvo.at[0], kvb.at[4], kv_send.at[4], kv_recv.at[4], dev(y_up, z, t)),
        5: copy(kvb.at[0], kvb.at[5], kv_send.at[5], kv_recv.at[5], dev(y_down, z, s)),
        6: copy(kvb.at[2], kvb.at[6], kv_send.at[6], kv_recv.at[6], dev(y_up, z, s)),
        7: copy(kvb.at[3], kvb.at[7], kv_send.at[7], kv_recv.at[7], dev(y_down, z, s)),
        9: copy(kvo.at[1], kvb.at[9], kv_send.at[9], kv_recv.at[9], partner),
    }
    for j in (2, 3, 1, 4, 5):
        kv[j].start()

    mine_rows = pl.ds(pl.multiple_of(s * HD, HD), HD)
    weights = {}
    for j in range(1, 8):
        weights[j] = copy(
            wo_hbm.at[mine_rows], w_o.at[j, mine_rows], w_send.at[j], w_recv.at[j],
            (p, chan_of(j)),
        )
    passed = {}
    for j in range(1, 8):
        passed[j] = copy(
            w_o.at[j, mine_rows], w_o.at[j, mine_rows], wx_send.at[j], wx_recv.at[j], partner
        )
    for j in (1, 2, 3):
        weights[j].start()

    step = 128
    loads[2].wait()

    def norm_rows(i, _):
        at = pl.ds(pl.multiple_of(i * step, step), step)
        normed[at, :] = normalize(tok[at, :].astype(F32)).astype(BF16)
        return 0

    lax.fori_loop(0, rows // step, norm_rows, 0)

    def project(w):
        return jnp.dot(normed[...], w[...], preferred_element_type=F32).astype(BF16)

    loads[3].wait()
    mine, other = split_heads(project(w_q).T)
    q = {}
    for h in (0, 1):
        qb[0, h] = mine[:, h * half : (h + 1) * half]
        qo[h] = other[:, h * half : (h + 1) * half]
    for h in (0, 1):
        for j, (from_ref, peer) in {
            2: (qb.at[0, h], dev(y, z_up, s)),
            3: (qo.at[h], dev(y, z_down, t)),
            4: (qo.at[h], dev(y, z_up, t)),
            5: (qb.at[0, h], dev(y, z_down, s)),
            1: (qo.at[h], partner),
            6: (qb.at[2, h], dev(y, z_up, s)),
            7: (qb.at[3, h], dev(y, z_down, s)),
        }.items():
            q[j, h] = copy(from_ref, qb.at[j, h], q_send.at[j, h], q_recv.at[j, h], peer)
        for j in (2, 3, 4, 5, 1):
            q[j, h].start()
    for j, w in enumerate((w_k, w_v)):
        loads[4 + j].wait()
        mine, other = split_heads(project(w).T)
        kvb[8, j] = mine
        kvo[1, j] = other
    kv[9].start()

    top[...] = jnp.full(top.shape, LOW, F32)
    total[...] = jnp.zeros(total.shape, F32)
    acc[...] = jnp.zeros(acc.shape, F32)

    def prepare_keys(u):
        key = kvb[u, 0]
        kk[u] = jnp.concatenate([key, key], axis=0).T

    def prepare_queries(f, h):
        scaled = qb[f, h].astype(F32) * SCALE
        high = scaled.astype(BF16)
        low = (scaled - high.astype(F32)).astype(BF16)
        qq[f, h] = jnp.concatenate([high, low], axis=0)

    def score(h, item, s_ref, b_ref):
        f, ua, ub = item
        first = jnp.dot(kk[ua], qq[f, h], preferred_element_type=F32)
        s_ref[:rows] = first
        second = jnp.dot(kk[ub], qq[f, h], preferred_element_type=F32)
        s_ref[rows:] = second
        b_ref[...] = jnp.maximum(
            jnp.max(first, axis=0, keepdims=True), jnp.max(second, axis=0, keepdims=True)
        )

    def absorb(h, item, s_ref, b_ref):
        f, ua, ub = item
        old = top[f, h]
        new = jnp.maximum(old, b_ref[...])
        rescale = jnp.exp2(old - new)
        first = jnp.exp2(s_ref[:rows] - new)
        second = jnp.exp2(s_ref[rows:] - new)
        total[f, h] = (
            total[f, h] * rescale
            + jnp.sum(first, axis=0, keepdims=True)
            + jnp.sum(second, axis=0, keepdims=True)
        )
        acc[f, h] = (
            acc[f, h] * rescale
            + jnp.dot(kvb[ua, 1], first.astype(BF16), preferred_element_type=F32)
            + jnp.dot(kvb[ub, 1], second.astype(BF16), preferred_element_type=F32)
        )
        top[f, h] = new

    def attend(h, count, item):
        score(h, item(0), s_a, b_a)

        def two(i, _):
            first, second = item(2 * i), item(2 * i + 1)
            third = item(jnp.minimum(2 * i + 2, count - 1))
            score(h, second, s_b, b_b)
            absorb(h, first, s_a, b_a)
            score(h, third, s_a, b_a)
            absorb(h, second, s_b, b_b)
            return 0

        lax.fori_loop(0, count // 2, two, 0)

    def block(h, f0, nf, g0, ng):
        def item(i):
            i = jnp.int32(i)
            u = 2 * (g0 + lax.rem(i, ng))
            return f0 + lax.div(i, ng), u, u + 1

        attend(h, nf * ng, item)

    def own_item(i):
        i = jnp.int32(i)
        return i, 8 * (1 - i), 1 + 8 * i

    def keys_ready(*units):
        for u in units:
            kv[u].wait_recv()
            if u in (2, 3):
                kv[u + 4].start()
            prepare_keys(u)

    def queries_ready(h, *units):
        for f in units:
            q[f, h].wait_recv()
            if f in (2, 3):
                q[f + 4, h].start()
            prepare_queries(f, h)

    targets = {
        6: (dev(y, z_up, s), 5),
        7: (dev(y, z_down, s), 6),
        2: (dev(y, z_down, s), 1),
        3: (dev(y, z_up, t), 2),
        4: (dev(y, z_down, t), 3),
        5: (dev(y, z_up, s), 4),
        1: (partner, 0),
    }
    back = {}
    for h in (0, 1):
        for f, (peer, slot) in targets.items():
            back[f, h] = (
                copy(
                    o_out.at[f, h], o_in.at[slot, h], o_send.at[f, h], o_recv.at[slot, h], peer
                ),
                copy(
                    stat_out.at[f, h], stat_in.at[slot, h], t_send.at[f, h],
                    t_recv.at[slot, h], peer,
                ),
            )

    def give(h, *units):
        for f in units:
            o_out[f, h] = acc[f, h].astype(BF16)
            stat_out[f, h, 0:1] = top[f, h]
            stat_out[f, h, 1:2] = total[f, h]
            for part in back[f, h]:
                part.start()

    def arrived(h, *units):
        for f in units:
            for part in back[f, h]:
                part.wait_recv()

    def merge(one, other):
        new = jnp.maximum(one[0], other[0])
        left, right = jnp.exp2(one[0] - new), jnp.exp2(other[0] - new)
        return (
            new,
            one[1] * left + other[1] * right,
            one[2] * left + other[2] * right,
        )

    def received(h, slot):
        return stat_in[slot, h, 0:1], stat_in[slot, h, 1:2], o_in[slot, h].astype(F32)

    def local(h, f):
        return top[f, h], total[f, h], acc[f, h]

    def pass_on(h):
        arrived(h, 6, 7)
        for f, slot in ((5, 5), (4, 6)):
            top[f, h], total[f, h], acc[f, h] = merge(local(h, f), received(h, slot))
        give(h, 4, 5)

    gathers = {}
    for h in (0, 1):
        for j in range(1, 8):
            gathers[j, h] = copy(
                att.at[h, 0], att.at[h, j], a_send.at[j, h], a_recv.at[j, h], (p, chan_of(j))
            )

    def finish(h):
        arrived(h, 1, 2, 3, 4, 5)
        _, sums, values = merge(merge(local(h, 0), received(h, 1)), received(h, 4))
        fin[s] = values / sums
        _, sums, values = merge(merge(received(h, 0), received(h, 2)), received(h, 3))
        fin[t] = values / sums
        att[h, 0] = jnp.concatenate([fin[0], fin[1]], axis=0).T.astype(BF16)
        for j in (5, 7, 4, 1, 3, 6, 2):
            gathers[j, h].start()

    scatters = {}
    for h in (0, 1):
        for j in range(1, 8):
            chunk = pl.ds(pl.multiple_of(chan_of(j) * share, 32), share)
            scatters[j, h] = copy(
                down.at[h, chunk], pieces.at[h, j], r_send.at[j, h], r_recv.at[j, h],
                (p, chan_of(j)),
            )
    my_chunk = pl.ds(pl.multiple_of(c * share, 32), share)

    def feed_forward(h):
        for j in range(1, 8):
            gathers[j, h].wait_recv()
        here = slice(h * half, (h + 1) * half)
        mixed = tok[here].astype(F32)
        for j in range(0, 8, 2):
            mixed += jnp.dot(
                jnp.concatenate([att[h, j], att[h, j + 1]], axis=1),
                w_o[j : j + 2].reshape(4 * HD, w_o.shape[2]),
                preferred_element_type=F32,
            )
        resid[h] = mixed

        def norm_again(i, _):
            at = pl.ds(pl.multiple_of(i * step, step), step)
            normed[at, :] = normalize(resid[h, at, :]).astype(BF16)
            return 0

        lax.fori_loop(0, half // step, norm_again, 0)
        inputs = normed[:half]
        values = jnp.dot(inputs, f_v[...], preferred_element_type=F32)
        gate = jnp.dot(inputs, f_g[...], preferred_element_type=F32)
        gate = 0.5 * gate * (1.0 + lax.erf(gate * math.sqrt(0.5)))
        gated = (values * gate).astype(BF16)
        result = jnp.dot(gated, f_d[...], preferred_element_type=F32)
        down[h] = result.astype(BF16).T
        for j in (5, 7, 4, 1, 3, 6, 2):
            scatters[j, h].start()
        turned[h] = resid[h].T

    def conclude(h):
        sums = turned[h, my_chunk] + down[h, my_chunk].astype(F32)
        for j in range(1, 8):
            scatters[j, h].wait_recv()
            sums += pieces[h, j].astype(F32)
        out[h * half : (h + 1) * half] = sums.T.astype(out.dtype)

    prepare_keys(0)
    prepare_keys(8)
    prepare_queries(0, 0)
    prepare_queries(0, 1)
    keys_ready(1, 9)
    queries_ready(0, 1)
    queries_ready(1, 1)
    attend(0, 2, own_item)
    attend(1, 2, own_item)
    keys_ready(2, 3)
    block(0, 0, 2, 1, 1)
    block(1, 0, 2, 1, 1)
    queries_ready(0, 2, 3)
    keys_ready(4, 5)
    block(0, 2, 2, 0, 3)
    queries_ready(0, 4, 5)
    queries_ready(1, 2, 3)
    block(0, 4, 2, 0, 3)
    queries_ready(0, 6, 7)
    keys_ready(6, 7)
    block(0, 6, 2, 0, 4)
    give(0, 6, 7)
    for j in (4, 5, 6, 7):
        weights[j].start()
    block(0, 2, 4, 3, 1)
    give(0, 2, 3)
    block(0, 0, 2, 2, 2)
    give(0, 1)
    queries_ready(1, 4, 5, 6, 7)
    block(1, 6, 2, 0, 4)
    give(1, 6, 7)
    pass_on(0)
    block(1, 2, 2, 0, 4)
    give(1, 2, 3)
    for j in (1, 2, 3):
        weights[j].wait_recv()
        passed[j].start()
    block(1, 4, 2, 0, 4)
    finish(0)
    pass_on(1)
    block(1, 0, 2, 2, 2)
    give(1, 1)
    for j in (4, 5, 6, 7):
        weights[j].wait_recv()
        passed[j].start()
    for part in loads[6:]:
        part.wait()
    for j in range(1, 8):
        passed[j].wait_recv()
    finish(1)
    feed_forward(0)
    feed_forward(1)
    conclude(0)
    conclude(1)

    for j in (1, 2, 3, 4, 5, 6, 7, 9):
        kv[j].wait_send()
    for j in range(1, 8):
        weights[j].wait_send()
        passed[j].wait_send()
        for h in (0, 1):
            q[j, h].wait_send()
            for part in back[j, h]:
                part.wait_send()
            gathers[j, h].wait_send()
            scatters[j, h].wait_send()


def per_device(
    tokens, stale_k, stale_v, w_query, w_key, w_value, w_out, ff_value, ff_gate, ff_down
):
    _, rows, width = tokens.shape
    half, hidden = rows // 2, ff_value.shape[1]
    share = width // lax.axis_size("chan")
    vmem, dma = pltpu.VMEM, pltpu.SemaphoreType.DMA
    result = pl.pallas_call(
        block_kernel,
        out_shape=jax.ShapeDtypeStruct((rows, share), BF16),
        in_specs=[pl.BlockSpec(memory_space=pl.ANY)] * 10,
        out_specs=pl.BlockSpec(memory_space=vmem),
        scratch_shapes=[
            vmem((rows, width), BF16),
            vmem((rows, 2 * HD), BF16),
            vmem((rows, 2 * HD), BF16),
            vmem((width, 2 * HD), BF16),
            vmem((width, 2 * HD), BF16),
            vmem((width, 2 * HD), BF16),
            vmem((8, 2 * HD, width), BF16),
            vmem((width, hidden), BF16),
            vmem((width, hidden), BF16),
            vmem((hidden, width), BF16),
            vmem((rows, width), BF16),
            vmem((10, 2, HD, rows), BF16),
            vmem((2, 2, HD, rows), BF16),
            vmem((8, 2, HD, half), BF16),
            vmem((2, HD, half), BF16),
            vmem((10, rows, 2 * HD), BF16),
            vmem((8, 2, 2 * HD, half), BF16),
            vmem((2 * rows, half), F32),
            vmem((2 * rows, half), F32),
            vmem((1, half), F32),
            vmem((1, half), F32),
            vmem((8, 2, 1, half), F32),
            vmem((8, 2, 1, half), F32),
            vmem((8, 2, HD, half), F32),
            vmem((8, 2, 2, half), F32),
            vmem((8, 2, HD, half), BF16),
            vmem((7, 2, HD, half), BF16),
            vmem((7, 2, 2, half), F32),
            vmem((2, HD, half), F32),
            vmem((2, 8, half, 2 * HD), BF16),
            vmem((2, half, width), F32),
            vmem((2, width, half), F32),
            vmem((2, width, half), BF16),
            vmem((2, 8, share, half), BF16),
            dma((10,)),
            dma((10,)), dma((10,)), dma((8, 2)), dma((8, 2)),
            dma((8, 2)), dma((7, 2)), dma((8, 2)), dma((7, 2)),
            dma((8,)), dma((8,)), dma((8,)), dma((8,)),
            dma((8, 2)), dma((8, 2)), dma((8, 2)), dma((8, 2)),
        ],
        compiler_params=pltpu.CompilerParams(collective_id=0, has_side_effects=True),
    )(
        tokens[0], stale_k[0], stale_v[0], w_query, w_key, w_value, w_out,
        ff_value, ff_gate, ff_down,
    )
    return result[None]


def solution(mesh):
    return jax.shard_map(
        per_device,
        mesh=mesh,
        in_specs=(
            P(None, "patch", None),
            P(None, "patch", "chan"),
            P(None, "patch", "chan"),
            P(None, "chan"),
            P(None, "chan"),
            P(None, "chan"),
            P("chan", None),
            P(None, "chan"),
            P(None, "chan"),
            P("chan", None),
        ),
        out_specs=P(None, "patch", "chan"),
        check_vma=False,
    )
```

```python
import functools
import math

import jax
import jax.numpy as jnp
from jax import lax
from jax.experimental import pallas as pl
from jax.experimental.pallas import tpu as pltpu
from jax.sharding import PartitionSpec as P

HD = 64
MESH = pl.DeviceIdType.MESH
F32 = jnp.float32
BF16 = jnp.bfloat16
LOW = -1e30
SCALE = math.log2(math.e) / math.sqrt(HD)


def normalize(values):
    mean = jnp.mean(values, axis=-1, keepdims=True)
    centered = values - mean
    var = jnp.mean(centered * centered, axis=-1, keepdims=True)
    return centered * lax.rsqrt(var + 1e-05)


def block_kernel(
    tok_hbm, k_hbm, v_hbm, wq_hbm, wk_hbm, wv_hbm, wo_hbm, fv_hbm, fg_hbm, fd_hbm, out,
    tok, k_in, v_in, w_q, w_k, w_v, w_o, f_v, f_g, f_d,
    normed, kvb, kvo, qb, qo, kk, qq, s_a, s_b, b_a, b_b,
    top, total, acc, stat_out, o_out, o_in, stat_in, fin,
    att, resid, turned, down, pieces,
    load, kv_send, kv_recv, q_send, q_recv, o_send, o_recv, t_send, t_recv,
    w_send, w_recv, wx_send, wx_recv, a_send, a_recv, r_send, r_recv,
):
    p, c = lax.axis_index("patch"), lax.axis_index("chan")
    s = lax.rem(p, 2)
    z = lax.rem(lax.div(p, 2), 4)
    y = lax.div(p, 8)
    t = 1 - s
    y_up, y_down = lax.rem(y + 1, 4), lax.rem(y + 3, 4)
    z_up, z_down = lax.rem(z + 1, 4), lax.rem(z + 3, 4)
    y_far, z_far = lax.rem(y + 2, 4), lax.rem(z + 2, 4)
    across, along = lax.div(c, 4), lax.rem(c, 4)
    rows = tok.shape[0]
    half = rows // 2
    share = out.shape[1]

    def dev(y, z, s):
        return ((y * 4 + z) * 2 + s, c)

    partner = dev(y, z, t)

    def chan_of(j):
        return lax.rem(across + j // 4, 2) * 4 + lax.rem(along + j % 4, 4)

    loads = [
        pltpu.make_async_copy(src, dst, load.at[i])
        for i, (src, dst) in enumerate(
            (
                (k_hbm, k_in), (v_hbm, v_in), (tok_hbm, tok), (wq_hbm, w_q),
                (wk_hbm, w_k), (wv_hbm, w_v), (wo_hbm, w_o.at[0]), (fv_hbm, f_v),
                (fg_hbm, f_g), (fd_hbm, f_d),
            )
        )
    ]
    for part in loads[:4]:
        part.start()

    barrier = pltpu.get_barrier_semaphore()
    peers = [partner]
    for core in (s, t):
        peers += [dev(y_up, z, core), dev(y_down, z, core)]
        peers += [dev(y, z_up, core), dev(y, z_down, core)]
        peers += [dev(y_far, z, core), dev(y, z_far, core)]
    peers += [(p, chan_of(j)) for j in range(1, 8)]
    for peer in peers:
        pl.semaphore_signal(barrier, inc=1, device_id=peer, device_id_type=MESH)

    def split_heads(values):
        first, second = values[:HD], values[HD:]
        mine = jnp.where(s == 0, first, second)
        other = jnp.where(s == 0, second, first)
        return mine, other

    def copy(src, dst, send, recv, peer):
        return pltpu.make_async_remote_copy(
            src_ref=src, dst_ref=dst, send_sem=send, recv_sem=recv,
            device_id=peer, device_id_type=MESH,
        )

    for j, ref in enumerate((k_in, v_in)):
        loads[j].wait()
        mine, other = split_heads(ref[...].T)
        kvb[0, j] = mine
        kvo[0, j] = other
    pl.semaphore_wait(barrier, len(peers))
    kv = {
        2: copy(kvb.at[0], kvb.at[2], kv_send.at[2], kv_recv.at[2], dev(y_up, z, s)),
        3: copy(kvo.at[0], kvb.at[3], kv_send.at[3], kv_recv.at[3], dev(y_down, z, t)),
        1: copy(kvo.at[0], kvb.at[1], kv_send.at[1], kv_recv.at[1], partner),
        4: copy(kvo.at[0], kvb.at[4], kv_send.at[4], kv_recv.at[4], dev(y_up, z, t)),
        5: copy(kvb.at[0], kvb.at[5], kv_send.at[5], kv_recv.at[5], dev(y_down, z, s)),
        6: copy(kvb.at[0], kvb.at[6], kv_send.at[6], kv_recv.at[6], dev(y_far, z, s)),
        7: copy(kvo.at[0], kvb.at[7], kv_send.at[7], kv_recv.at[7], dev(y_far, z, t)),
        9: copy(kvo.at[1], kvb.at[9], kv_send.at[9], kv_recv.at[9], partner),
    }
    for j in (2, 3, 1, 4, 5, 6, 7):
        kv[j].start()

    mine_rows = pl.ds(pl.multiple_of(s * HD, HD), HD)
    weights = {}
    for j in range(1, 8):
        weights[j] = copy(
            wo_hbm.at[mine_rows] if j < 5 else w_o.at[4, mine_rows],
            w_o.at[j, mine_rows], w_send.at[j], w_recv.at[j],
            (p, chan_of(j if j < 5 else j - 4)),
        )
    passed = {}
    for j in range(1, 8):
        passed[j] = copy(
            w_o.at[j, mine_rows], w_o.at[j, mine_rows], wx_send.at[j], wx_recv.at[j], partner
        )
    for part in loads[4:]:
        part.start()
    for j in (1, 3, 2):
        weights[j].start()

    step = 128
    loads[2].wait()

    def norm_rows(i, _):
        at = pl.ds(pl.multiple_of(i * step, step), step)
        normed[at, :] = normalize(tok[at, :].astype(F32)).astype(BF16)
        return 0

    def project(w, here):
        result = jnp.dot(normed[here], w[...], preferred_element_type=F32)
        return split_heads(result.astype(BF16).T)

    loads[3].wait()
    q = {}
    for h in (0, 1):
        for j, (from_ref, peer) in {
            2: (qb.at[0, h], dev(y, z_up, s)),
            3: (qo.at[h], dev(y, z_down, t)),
            4: (qo.at[h], dev(y, z_up, t)),
            5: (qb.at[0, h], dev(y, z_down, s)),
            1: (qo.at[h], partner),
            6: (qb.at[0, h], dev(y, z_far, s)),
            7: (qo.at[h], dev(y, z_far, t)),
        }.items():
            q[j, h] = copy(from_ref, qb.at[j, h], q_send.at[j, h], q_recv.at[j, h], peer)
    for h in (0, 1):
        lax.fori_loop(h * half // step, (h + 1) * half // step, norm_rows, 0)
        qb[0, h], qo[h] = project(w_q, slice(h * half, (h + 1) * half))
        for j in (1, 2, 3, 4, 5, 6, 7):
            q[j, h].start()
    weights[4].start()
    for j, w in enumerate((w_k, w_v)):
        loads[4 + j].wait()
        kvb[8, j], kvo[1, j] = project(w, slice(0, rows))
    kv[9].start()

    top[...] = jnp.full(top.shape, LOW, F32)
    total[...] = jnp.zeros(total.shape, F32)
    acc[...] = jnp.zeros(acc.shape, F32)

    def prepare_keys(u):
        key = kvb[u, 0]
        kk[u] = jnp.concatenate([key, key], axis=0).T

    def prepare_queries(f, h):
        scaled = qb[f, h].astype(F32) * SCALE
        high = scaled.astype(BF16)
        low = (scaled - high.astype(F32)).astype(BF16)
        qq[f, h] = jnp.concatenate([high, low], axis=0)

    def score(h, item, s_ref, b_ref):
        f, ua, ub = item
        first = jnp.dot(kk[ua], qq[f, h], preferred_element_type=F32)
        s_ref[:rows] = first
        second = jnp.dot(kk[ub], qq[f, h], preferred_element_type=F32)
        s_ref[rows:] = second
        b_ref[...] = jnp.maximum(
            jnp.max(first, axis=0, keepdims=True), jnp.max(second, axis=0, keepdims=True)
        )

    def absorb(h, item, s_ref, b_ref):
        f, ua, ub = item
        old = top[f, h]
        new = jnp.maximum(old, b_ref[...])
        rescale = jnp.exp2(old - new)
        first = jnp.exp2(s_ref[:rows] - new)
        second = jnp.exp2(s_ref[rows:] - new)
        total[f, h] = (
            total[f, h] * rescale
            + jnp.sum(first, axis=0, keepdims=True)
            + jnp.sum(second, axis=0, keepdims=True)
        )
        acc[f, h] = (
            acc[f, h] * rescale
            + jnp.dot(kvb[ua, 1], first.astype(BF16), preferred_element_type=F32)
            + jnp.dot(kvb[ub, 1], second.astype(BF16), preferred_element_type=F32)
        )
        top[f, h] = new

    def attend(h, count, item):
        score(h, item(0), s_a, b_a)

        def two(i, _):
            first, second = item(2 * i), item(2 * i + 1)
            third = item(jnp.minimum(2 * i + 2, count - 1))
            score(h, second, s_b, b_b)
            absorb(h, first, s_a, b_a)
            score(h, third, s_a, b_a)
            absorb(h, second, s_b, b_b)
            return 0

        lax.fori_loop(0, count // 2, two, 0)

    def block(h, f0, nf, g0, ng):
        def item(i):
            i = jnp.int32(i)
            u = 2 * (g0 + lax.rem(i, ng))
            return f0 + lax.div(i, ng), u, u + 1

        attend(h, nf * ng, item)

    def own_item(i):
        i = jnp.int32(i)
        return i, 8 * (1 - i), 1 + 8 * i

    def keys_ready(*units):
        for u in units:
            kv[u].wait_recv()
            prepare_keys(u)

    def queries_ready(h, *units):
        for f in units:
            q[f, h].wait_recv()
            prepare_queries(f, h)

    targets = {
        6: (dev(y, z_far, s), 5),
        7: (dev(y, z_far, t), 6),
        2: (dev(y, z_down, s), 1),
        3: (dev(y, z_up, t), 2),
        4: (dev(y, z_down, t), 3),
        5: (dev(y, z_up, s), 4),
        1: (partner, 0),
    }
    back = {}
    for h in (0, 1):
        for f, (peer, slot) in targets.items():
            back[f, h] = (
                copy(
                    o_out.at[f, h], o_in.at[slot, h], o_send.at[f, h], o_recv.at[slot, h], peer
                ),
                copy(
                    stat_out.at[f, h], stat_in.at[slot, h], t_send.at[f, h],
                    t_recv.at[slot, h], peer,
                ),
            )

    def give(h, *units):
        for f in units:
            o_out[f, h] = acc[f, h].astype(BF16)
            stat_out[f, h, 0:1] = top[f, h]
            stat_out[f, h, 1:2] = total[f, h]
            for part in back[f, h]:
                part.start()

    def arrived(h, *units):
        for f in units:
            for part in back[f, h]:
                part.wait_recv()

    def merge(one, other):
        new = jnp.maximum(one[0], other[0])
        left, right = jnp.exp2(one[0] - new), jnp.exp2(other[0] - new)
        return (
            new,
            one[1] * left + other[1] * right,
            one[2] * left + other[2] * right,
        )

    def received(h, slot):
        return stat_in[slot, h, 0:1], stat_in[slot, h, 1:2], o_in[slot, h].astype(F32)

    def local(h, f):
        return top[f, h], total[f, h], acc[f, h]

    gathers = {}
    for h in (0, 1):
        for j in range(1, 8):
            relay = h == 0 and j > 4
            gathers[j, h] = copy(
                att.at[h, 4 if relay else 0], att.at[h, j], a_send.at[j, h], a_recv.at[j, h],
                (p, chan_of(j - 4 if relay else j)),
            )

    def finish(h):
        arrived(h, 1, 2, 3, 4, 5, 6, 7)
        for head, parts in (
            (s, (local(h, 0), received(h, 1), received(h, 4), received(h, 5))),
            (t, (received(h, 0), received(h, 2), received(h, 3), received(h, 6))),
        ):
            _, sums, values = functools.reduce(merge, parts)
            fin[head] = values / sums
        att[h, 0] = jnp.concatenate([fin[0], fin[1]], axis=0).T.astype(BF16)
        for j in (4, 1, 3, 2) if h == 0 else (5, 7, 4, 1, 3, 6, 2):
            gathers[j, h].start()

    scatters = {}
    for h in (0, 1):
        for j in range(1, 8):
            chunk = pl.ds(pl.multiple_of(chan_of(j) * share, 32), share)
            scatters[j, h] = copy(
                down.at[h, chunk], pieces.at[h, j], r_send.at[j, h], r_recv.at[j, h],
                (p, chan_of(j)),
            )
    my_chunk = pl.ds(pl.multiple_of(c * share, 32), share)

    def feed_forward(h):
        for j in range(1, 8):
            if h == 1 or j != 4:
                gathers[j, h].wait_recv()
        here = slice(h * half, (h + 1) * half)
        mixed = tok[here].astype(F32)
        for j in range(0, 8, 2):
            mixed += jnp.dot(
                jnp.concatenate([att[h, j], att[h, j + 1]], axis=1),
                w_o[j : j + 2].reshape(4 * HD, w_o.shape[2]),
                preferred_element_type=F32,
            )
        resid[h] = mixed

        def norm_again(i, _):
            at = pl.ds(pl.multiple_of(i * step, step), step)
            normed[at, :] = normalize(resid[h, at, :]).astype(BF16)
            return 0

        lax.fori_loop(0, half // step, norm_again, 0)
        inputs = normed[:half]
        values = jnp.dot(inputs, f_v[...], preferred_element_type=F32)
        gate = jnp.dot(inputs, f_g[...], preferred_element_type=F32)
        gate = 0.5 * gate * (1.0 + lax.erf(gate * math.sqrt(0.5)))
        gated = (values * gate).astype(BF16)
        result = jnp.dot(gated, f_d[...], preferred_element_type=F32)
        down[h] = result.astype(BF16).T
        for j in (5, 7, 4, 1, 3, 6, 2):
            scatters[j, h].start()
        turned[h] = resid[h].T

    def conclude(h):
        sums = turned[h, my_chunk] + down[h, my_chunk].astype(F32)
        for j in range(1, 8):
            scatters[j, h].wait_recv()
            sums += pieces[h, j].astype(F32)
        out[h * half : (h + 1) * half] = sums.T.astype(out.dtype)

    prepare_keys(0)
    prepare_keys(8)
    prepare_queries(0, 0)
    prepare_queries(0, 1)
    keys_ready(1, 9)
    queries_ready(0, 1)
    queries_ready(1, 1)
    attend(0, 2, own_item)
    attend(1, 2, own_item)
    keys_ready(2, 3)
    block(0, 0, 2, 1, 1)
    block(1, 0, 2, 1, 1)
    queries_ready(0, 2, 3)
    keys_ready(4, 5)
    block(0, 2, 2, 0, 3)
    queries_ready(0, 4, 5)
    block(0, 4, 2, 0, 3)
    queries_ready(0, 6, 7)
    keys_ready(6, 7)
    block(0, 6, 2, 0, 4)
    give(0, 6, 7)
    block(0, 2, 4, 3, 1)
    give(0, 2, 3, 4, 5)
    block(0, 0, 2, 2, 2)
    give(0, 1)
    weights[4].wait_recv()
    for j in (5, 7, 6):
        weights[j].start()
    queries_ready(1, 2, 3, 4, 5, 6, 7)
    block(1, 6, 2, 0, 4)
    give(1, 6, 7)
    for j in (1, 2, 3):
        weights[j].wait_recv()
    for j in (1, 2, 3, 4):
        passed[j].start()
    block(1, 2, 2, 0, 4)
    give(1, 2, 3)
    finish(0)
    block(1, 4, 2, 0, 4)
    give(1, 4, 5)
    block(1, 0, 2, 2, 2)
    give(1, 1)
    gathers[4, 0].wait_recv()
    for j in (5, 7, 6):
        gathers[j, 0].start()
        weights[j].wait_recv()
        passed[j].start()
    for part in loads[6:]:
        part.wait()
    for j in range(1, 8):
        passed[j].wait_recv()
    finish(1)
    feed_forward(0)
    feed_forward(1)
    conclude(0)
    conclude(1)

    for j in (1, 2, 3, 4, 5, 6, 7, 9):
        kv[j].wait_send()
    for j in range(1, 8):
        weights[j].wait_send()
        passed[j].wait_send()
        for h in (0, 1):
            q[j, h].wait_send()
            for part in back[j, h]:
                part.wait_send()
            gathers[j, h].wait_send()
            scatters[j, h].wait_send()


def per_device(
    tokens, stale_k, stale_v, w_query, w_key, w_value, w_out, ff_value, ff_gate, ff_down
):
    _, rows, width = tokens.shape
    half, hidden = rows // 2, ff_value.shape[1]
    share = width // lax.axis_size("chan")
    vmem, dma = pltpu.VMEM, pltpu.SemaphoreType.DMA
    result = pl.pallas_call(
        block_kernel,
        out_shape=jax.ShapeDtypeStruct((rows, share), BF16),
        in_specs=[pl.BlockSpec(memory_space=pl.ANY)] * 10,
        out_specs=pl.BlockSpec(memory_space=vmem),
        scratch_shapes=[
            vmem((rows, width), BF16),
            vmem((rows, 2 * HD), BF16),
            vmem((rows, 2 * HD), BF16),
            vmem((width, 2 * HD), BF16),
            vmem((width, 2 * HD), BF16),
            vmem((width, 2 * HD), BF16),
            vmem((8, 2 * HD, width), BF16),
            vmem((width, hidden), BF16),
            vmem((width, hidden), BF16),
            vmem((hidden, width), BF16),
            vmem((rows, width), BF16),
            vmem((10, 2, HD, rows), BF16),
            vmem((2, 2, HD, rows), BF16),
            vmem((8, 2, HD, half), BF16),
            vmem((2, HD, half), BF16),
            vmem((10, rows, 2 * HD), BF16),
            vmem((8, 2, 2 * HD, half), BF16),
            vmem((2 * rows, half), F32),
            vmem((2 * rows, half), F32),
            vmem((1, half), F32),
            vmem((1, half), F32),
            vmem((8, 2, 1, half), F32),
            vmem((8, 2, 1, half), F32),
            vmem((8, 2, HD, half), F32),
            vmem((8, 2, 2, half), F32),
            vmem((8, 2, HD, half), BF16),
            vmem((7, 2, HD, half), BF16),
            vmem((7, 2, 2, half), F32),
            vmem((2, HD, half), F32),
            vmem((2, 8, half, 2 * HD), BF16),
            vmem((2, half, width), F32),
            vmem((2, width, half), F32),
            vmem((2, width, half), BF16),
            vmem((2, 8, share, half), BF16),
            dma((10,)),
            dma((10,)), dma((10,)), dma((8, 2)), dma((8, 2)),
            dma((8, 2)), dma((7, 2)), dma((8, 2)), dma((7, 2)),
            dma((8,)), dma((8,)), dma((8,)), dma((8,)),
            dma((8, 2)), dma((8, 2)), dma((8, 2)), dma((8, 2)),
        ],
        compiler_params=pltpu.CompilerParams(collective_id=0, has_side_effects=True),
    )(
        tokens[0], stale_k[0], stale_v[0], w_query, w_key, w_value, w_out,
        ff_value, ff_gate, ff_down,
    )
    return result[None]


def solution(mesh):
    return jax.shard_map(
        per_device,
        mesh=mesh,
        in_specs=(
            P(None, "patch", None),
            P(None, "patch", "chan"),
            P(None, "patch", "chan"),
            P(None, "chan"),
            P(None, "chan"),
            P(None, "chan"),
            P("chan", None),
            P(None, "chan"),
            P(None, "chan"),
            P("chan", None),
        ),
        out_specs=P(None, "patch", "chan"),
        check_vma=False,
    )
```

```python
import functools
import math

import jax
import jax.numpy as jnp
from jax import lax
from jax.experimental import pallas as pl
from jax.experimental.pallas import tpu as pltpu
from jax.sharding import PartitionSpec as P

HD = 64
MESH = pl.DeviceIdType.MESH
F32 = jnp.float32
BF16 = jnp.bfloat16
LOW = -1e30
SCALE = math.log2(math.e) / math.sqrt(HD)


def normalize(values):
    mean = jnp.mean(values, axis=-1, keepdims=True)
    centered = values - mean
    var = jnp.mean(centered * centered, axis=-1, keepdims=True)
    return centered * lax.rsqrt(var + 1e-05)


def block_kernel(
    tok_hbm, k_hbm, v_hbm, wq_hbm, wk_hbm, wv_hbm, wo_hbm, fv_hbm, fg_hbm, fd_hbm, out,
    tok, k_in, v_in, w_q, w_kv, w_o, f_vg, f_d,
    normed, kvb, kvo, qb, qo, kk, qq, s_a, s_b, b_a, b_b,
    top, total, acc, stat_out, o_out, o_in, stat_in, fin,
    att, resid, turned, down, pieces,
    load, kv_send, kv_recv, q_send, q_recv, o_send, o_recv, t_send, t_recv,
    w_send, w_recv, wx_send, wx_recv, a_send, a_recv, r_send, r_recv,
):
    p, c = lax.axis_index("patch"), lax.axis_index("chan")
    s = lax.rem(p, 2)
    z = lax.rem(lax.div(p, 2), 4)
    y = lax.div(p, 8)
    t = 1 - s
    y_up, y_down = lax.rem(y + 1, 4), lax.rem(y + 3, 4)
    z_up, z_down = lax.rem(z + 1, 4), lax.rem(z + 3, 4)
    y_far, z_far = lax.rem(y + 2, 4), lax.rem(z + 2, 4)
    across, along = lax.div(c, 4), lax.rem(c, 4)
    rows = tok.shape[0]
    half = rows // 2
    share = out.shape[0]
    hidden = f_d.shape[0]

    def dev(y, z, s):
        return ((y * 4 + z) * 2 + s, c)

    partner = dev(y, z, t)

    def chan_of(j):
        return lax.rem(across + j // 4, 2) * 4 + lax.rem(along + j % 4, 4)

    loads = [
        pltpu.make_async_copy(src, dst, load.at[i])
        for i, (src, dst) in enumerate(
            (
                (k_hbm, k_in), (v_hbm, v_in), (tok_hbm, tok), (wq_hbm, w_q),
                (wk_hbm, w_kv.at[:, : 2 * HD]), (wv_hbm, w_kv.at[:, 2 * HD :]), (wo_hbm, w_o.at[0]),
                (fv_hbm, f_vg.at[:, :hidden]), (fg_hbm, f_vg.at[:, hidden:]), (fd_hbm, f_d),
            )
        )
    ]
    for part in loads[:4]:
        part.start()

    barrier = pltpu.get_barrier_semaphore()
    peers = [partner]
    for core in (s, t):
        peers += [dev(y_up, z, core), dev(y_down, z, core)]
        peers += [dev(y, z_up, core), dev(y, z_down, core)]
        peers += [dev(y_far, z, core), dev(y, z_far, core)]
    peers += [(p, chan_of(j)) for j in range(1, 8)]
    for peer in peers:
        pl.semaphore_signal(barrier, inc=1, device_id=peer, device_id_type=MESH)

    def split_heads(values):
        first, second = values[:HD], values[HD:]
        mine = jnp.where(s == 0, first, second)
        other = jnp.where(s == 0, second, first)
        return mine, other

    def copy(src, dst, send, recv, peer):
        return pltpu.make_async_remote_copy(
            src_ref=src, dst_ref=dst, send_sem=send, recv_sem=recv,
            device_id=peer, device_id_type=MESH,
        )

    for j, ref in enumerate((k_in, v_in)):
        loads[j].wait()
        mine, other = split_heads(ref[...].T)
        kvb[0, j] = mine
        kvo[0, j] = other
    pl.semaphore_wait(barrier, len(peers))
    kv = {
        2: copy(kvb.at[0], kvb.at[2], kv_send.at[2], kv_recv.at[2], dev(y_up, z, s)),
        3: copy(kvo.at[0], kvb.at[3], kv_send.at[3], kv_recv.at[3], dev(y_down, z, t)),
        1: copy(kvo.at[0], kvb.at[1], kv_send.at[1], kv_recv.at[1], partner),
        4: copy(kvo.at[0], kvb.at[4], kv_send.at[4], kv_recv.at[4], dev(y_up, z, t)),
        5: copy(kvb.at[0], kvb.at[5], kv_send.at[5], kv_recv.at[5], dev(y_down, z, s)),
        6: copy(kvb.at[0], kvb.at[6], kv_send.at[6], kv_recv.at[6], dev(y_far, z, s)),
        7: copy(kvo.at[0], kvb.at[7], kv_send.at[7], kv_recv.at[7], dev(y_far, z, t)),
        9: copy(kvo.at[1], kvb.at[9], kv_send.at[9], kv_recv.at[9], partner),
    }
    for j in (2, 3, 1, 4, 5, 6, 7):
        kv[j].start()

    mine_rows = pl.ds(pl.multiple_of(s * HD, HD), HD)
    weights = {}
    for j in range(1, 8):
        weights[j] = copy(
            wo_hbm.at[mine_rows] if j < 5 else w_o.at[4, mine_rows],
            w_o.at[j, mine_rows], w_send.at[j], w_recv.at[j],
            (p, chan_of(j if j < 5 else j - 4)),
        )
    passed = {}
    for j in range(1, 8):
        passed[j] = copy(
            w_o.at[j, mine_rows], w_o.at[j, mine_rows], wx_send.at[j], wx_recv.at[j], partner
        )
    for part in loads[4:]:
        part.start()
    for j in (1, 3, 2):
        weights[j].start()

    step = 128
    loads[2].wait()

    def norm_rows(i, _):
        at = pl.ds(pl.multiple_of(i * step, step), step)
        normed[at, :] = normalize(tok[at, :].astype(F32)).astype(BF16)
        return 0

    def project(w, here):
        result = jnp.dot(normed[here], w[...], preferred_element_type=F32)
        return result.astype(BF16).T

    loads[3].wait()
    q = {}
    for h in (0, 1):
        for j, (from_ref, peer) in {
            2: (qb.at[0, h], dev(y, z_up, s)),
            3: (qo.at[h], dev(y, z_down, t)),
            4: (qo.at[h], dev(y, z_up, t)),
            5: (qb.at[0, h], dev(y, z_down, s)),
            1: (qo.at[h], partner),
            6: (qb.at[0, h], dev(y, z_far, s)),
            7: (qo.at[h], dev(y, z_far, t)),
        }.items():
            q[j, h] = copy(from_ref, qb.at[j, h], q_send.at[j, h], q_recv.at[j, h], peer)
    for h in (0, 1):
        lax.fori_loop(h * half // step, (h + 1) * half // step, norm_rows, 0)
        qb[0, h], qo[h] = split_heads(project(w_q, slice(h * half, (h + 1) * half)))
        for j in (1, 2, 3, 4, 5, 6, 7):
            q[j, h].start()
        if h == 0:
            weights[4].start()
    loads[4].wait()
    loads[5].wait()
    both = project(w_kv, slice(0, rows))
    for j in (0, 1):
        kvb[8, j], kvo[1, j] = split_heads(both[j * 2 * HD : (j + 1) * 2 * HD])
    kv[9].start()

    top[...] = jnp.full(top.shape, LOW, F32)
    total[...] = jnp.zeros(total.shape, F32)
    acc[...] = jnp.zeros(acc.shape, F32)

    def prepare_keys(u):
        key = kvb[u, 0]
        kk[u] = jnp.concatenate([key, key], axis=0).T

    def prepare_queries(f, h):
        scaled = qb[f, h].astype(F32) * SCALE
        high = scaled.astype(BF16)
        low = (scaled - high.astype(F32)).astype(BF16)
        qq[f, h] = jnp.concatenate([high, low], axis=0)

    def score(item, s_ref, b_ref):
        h, pair, *units = item
        for side, u in enumerate(units):
            values = jnp.dot(kk[u], qq[2 * pair + side, h], preferred_element_type=F32)
            s_ref[side] = values
            b_ref[side] = jnp.max(values, axis=0, keepdims=True)

    def absorb(item, s_ref, b_ref):
        h, pair, *units = item
        for side, u in enumerate(units):
            f = 2 * pair + side
            old = top[f, h]
            new = jnp.maximum(old, b_ref[side])
            rescale = jnp.exp2(old - new)
            weights = jnp.exp2(s_ref[side] - new)
            total[f, h] = total[f, h] * rescale + jnp.sum(weights, axis=0, keepdims=True)
            acc[f, h] = acc[f, h] * rescale + jnp.dot(
                kvb[u, 1], weights.astype(BF16), preferred_element_type=F32
            )
            top[f, h] = new

    def block(h, first_pair, pairs, first_unit, units):
        def item(i):
            i = jnp.int32(i)
            u = first_unit + lax.rem(i, units)
            return jnp.int32(h), first_pair + lax.div(i, units), u, u

        return pairs * units, item

    def own_block(h):
        def item(i):
            i = jnp.int32(i)
            return jnp.int32(h), jnp.int32(0), 8 - 7 * i, 9 * i

        return 2, item

    def attend(this, then=None, started=False):
        count, item = this
        if not started:
            score(item(0), s_a, b_a)
        following = item(count - 1) if then is None else then[1](0)

        def two(i, _):
            first, second = item(2 * i), item(2 * i + 1)
            more = 2 * i + 2 < count
            third = tuple(
                jnp.where(more, inner, after)
                for inner, after in zip(item(2 * i + 2), following)
            )
            score(second, s_b, b_b)
            absorb(first, s_a, b_a)
            score(third, s_a, b_a)
            absorb(second, s_b, b_b)
            return 0

        lax.fori_loop(0, count // 2, two, 0)

    def keys_ready(*units):
        for u in units:
            kv[u].wait_recv()
            prepare_keys(u)

    def queries_ready(h, *units):
        for f in units:
            q[f, h].wait_recv()
            prepare_queries(f, h)

    targets = {
        6: (dev(y, z_far, s), 5),
        7: (dev(y, z_far, t), 6),
        2: (dev(y, z_down, s), 1),
        3: (dev(y, z_up, t), 2),
        4: (dev(y, z_down, t), 3),
        5: (dev(y, z_up, s), 4),
        1: (partner, 0),
    }
    back = {}
    for h in (0, 1):
        for f, (peer, slot) in targets.items():
            back[f, h] = (
                copy(
                    o_out.at[f, h], o_in.at[slot, h], o_send.at[f, h], o_recv.at[slot, h], peer
                ),
                copy(
                    stat_out.at[f, h], stat_in.at[slot, h], t_send.at[f, h],
                    t_recv.at[slot, h], peer,
                ),
            )

    def give(h, *units):
        for f in units:
            o_out[f, h] = acc[f, h].astype(BF16)
            stat_out[f, h, 0:1] = top[f, h]
            stat_out[f, h, 1:2] = total[f, h]
            for part in back[f, h]:
                part.start()

    def arrived(h, *units):
        for f in units:
            for part in back[f, h]:
                part.wait_recv()

    def merge(one, other):
        new = jnp.maximum(one[0], other[0])
        left, right = jnp.exp2(one[0] - new), jnp.exp2(other[0] - new)
        return (
            new,
            one[1] * left + other[1] * right,
            one[2] * left + other[2] * right,
        )

    def received(h, slot):
        return stat_in[slot, h, 0:1], stat_in[slot, h, 1:2], o_in[slot, h].astype(F32)

    def local(h, f):
        return top[f, h], total[f, h], acc[f, h]

    gathers = {}
    for h in (0, 1):
        for j in range(1, 8):
            relay = h == 0 and j > 4
            gathers[j, h] = copy(
                att.at[h, 4 if relay else 0], att.at[h, j], a_send.at[j, h], a_recv.at[j, h],
                (p, chan_of(j - 4 if relay else j)),
            )

    def finish(h):
        arrived(h, 1, 2, 3, 4, 5, 6, 7)
        for head, parts in (
            (s, (local(h, 0), received(h, 1), received(h, 4), received(h, 5))),
            (t, (received(h, 0), received(h, 2), received(h, 3), received(h, 6))),
        ):
            _, sums, values = functools.reduce(merge, parts)
            fin[head] = values / sums
        att[h, 0] = jnp.concatenate([fin[0], fin[1]], axis=0).T.astype(BF16)
        for j in (4, 1, 3, 2) if h == 0 else (5, 7, 4, 1, 3, 6, 2):
            gathers[j, h].start()

    scatters = {}
    for h in (0, 1):
        for j in range(1, 8):
            chunk = pl.ds(pl.multiple_of(chan_of(j) * share, 32), share)
            scatters[j, h] = copy(
                down.at[h, chunk], pieces.at[h, j], r_send.at[j, h], r_recv.at[j, h],
                (p, chan_of(j)),
            )
    my_chunk = pl.ds(pl.multiple_of(c * share, 32), share)

    def feed_forward(h):
        for j in range(1, 8):
            if h == 1 or j != 4:
                gathers[j, h].wait_recv()
        here = slice(h * half, (h + 1) * half)
        mixed = tok[here].astype(F32)
        for j in range(0, 8, 2):
            mixed += jnp.dot(
                jnp.concatenate([att[h, j], att[h, j + 1]], axis=1),
                w_o[j : j + 2].reshape(4 * HD, w_o.shape[2]),
                preferred_element_type=F32,
            )
        resid[h] = mixed

        def norm_again(i, _):
            at = pl.ds(pl.multiple_of(i * step, step), step)
            normed[at, :] = normalize(resid[h, at, :]).astype(BF16)
            return 0

        lax.fori_loop(0, half // step, norm_again, 0)
        inputs = normed[:half]
        both = jnp.dot(inputs, f_vg[...], preferred_element_type=F32)
        values, gate = both[:, :hidden], both[:, hidden:]
        gate = 0.5 * gate * (1.0 + lax.erf(gate * math.sqrt(0.5)))
        gated = (values * gate).astype(BF16)
        result = jnp.dot(gated, f_d[...], preferred_element_type=F32)
        down[h] = result.astype(BF16).T
        for j in (5, 7, 4, 1, 3, 6, 2):
            scatters[j, h].start()

    def conclude(h):
        turned[h] = resid[h].T
        sums = turned[h, my_chunk] + down[h, my_chunk].astype(F32)
        for j in range(1, 8):
            scatters[j, h].wait_recv()
            sums += pieces[h, j].astype(F32)
        out[:, h * half : (h + 1) * half] = sums.astype(out.dtype)

    prepare_keys(0)
    prepare_keys(8)
    prepare_queries(0, 0)
    prepare_queries(0, 1)
    keys_ready(1, 9)
    queries_ready(0, 1)
    queries_ready(1, 1)
    attend(own_block(0), own_block(1))
    attend(own_block(1), started=True)
    keys_ready(2, 3)
    attend(block(0, 0, 1, 2, 2), block(1, 0, 1, 2, 2))
    attend(block(1, 0, 1, 2, 2), started=True)
    queries_ready(0, 2, 3)
    attend(block(0, 1, 1, 0, 4))
    keys_ready(4, 5)
    queries_ready(0, 4, 5)
    attend(block(0, 1, 1, 4, 2), block(0, 2, 1, 0, 6))
    attend(block(0, 2, 1, 0, 6), started=True)
    queries_ready(0, 6, 7)
    keys_ready(6, 7)
    ahead = [
        block(0, 1, 1, 6, 2), block(0, 2, 1, 6, 2), block(0, 3, 1, 0, 8), block(0, 0, 1, 4, 4),
        block(1, 3, 1, 0, 8), block(1, 1, 1, 0, 8), block(1, 2, 1, 0, 8), block(1, 0, 1, 4, 4),
    ]
    attend(ahead[0], ahead[1])
    give(0, 2, 3)
    attend(ahead[1], ahead[2], started=True)
    give(0, 4, 5)
    attend(ahead[2], ahead[3], started=True)
    give(0, 6, 7)
    attend(ahead[3], started=True)
    give(0, 1)
    weights[4].wait_recv()
    for j in (5, 7, 6):
        weights[j].start()
    queries_ready(1, 2, 3, 4, 5, 6, 7)
    attend(ahead[4], ahead[5])
    give(1, 6, 7)
    for j in (1, 2, 3):
        weights[j].wait_recv()
    for j in (1, 2, 3, 4):
        passed[j].start()
    attend(ahead[5], ahead[6], started=True)
    give(1, 2, 3)
    finish(0)
    attend(ahead[6], ahead[7], started=True)
    give(1, 4, 5)
    attend(ahead[7], started=True)
    give(1, 1)
    gathers[4, 0].wait_recv()
    for j in (5, 7, 6):
        gathers[j, 0].start()
    for j in (5, 7, 6):
        weights[j].wait_recv()
        passed[j].start()
    finish(1)
    for part in loads[6:]:
        part.wait()
    for j in range(1, 8):
        passed[j].wait_recv()
    feed_forward(0)
    feed_forward(1)
    conclude(0)
    conclude(1)

    for j in (1, 2, 3, 4, 5, 6, 7, 9):
        kv[j].wait_send()
    for j in range(1, 8):
        weights[j].wait_send()
        passed[j].wait_send()
        for h in (0, 1):
            q[j, h].wait_send()
            for part in back[j, h]:
                part.wait_send()
            gathers[j, h].wait_send()
            scatters[j, h].wait_send()


def per_device(
    tokens, stale_k, stale_v, w_query, w_key, w_value, w_out, ff_value, ff_gate, ff_down
):
    _, rows, width = tokens.shape
    half, hidden = rows // 2, ff_value.shape[1]
    share = width // lax.axis_size("chan")
    vmem, dma = pltpu.VMEM, pltpu.SemaphoreType.DMA
    result = pl.pallas_call(
        block_kernel,
        out_shape=jax.ShapeDtypeStruct((share, rows), BF16),
        in_specs=[pl.BlockSpec(memory_space=pl.ANY)] * 10,
        out_specs=pl.BlockSpec(memory_space=vmem),
        scratch_shapes=[
            vmem((rows, width), BF16),
            vmem((rows, 2 * HD), BF16),
            vmem((rows, 2 * HD), BF16),
            vmem((width, 2 * HD), BF16),
            vmem((width, 4 * HD), BF16),
            vmem((8, 2 * HD, width), BF16),
            vmem((width, 2 * hidden), BF16),
            vmem((hidden, width), BF16),
            vmem((rows, width), BF16),
            vmem((10, 2, HD, rows), BF16),
            vmem((2, 2, HD, rows), BF16),
            vmem((8, 2, HD, half), BF16),
            vmem((2, HD, half), BF16),
            vmem((10, rows, 2 * HD), BF16),
            vmem((8, 2, 2 * HD, half), BF16),
            vmem((2, rows, half), F32),
            vmem((2, rows, half), F32),
            vmem((2, 1, half), F32),
            vmem((2, 1, half), F32),
            vmem((8, 2, 1, half), F32),
            vmem((8, 2, 1, half), F32),
            vmem((8, 2, HD, half), F32),
            vmem((8, 2, 2, half), F32),
            vmem((8, 2, HD, half), BF16),
            vmem((7, 2, HD, half), BF16),
            vmem((7, 2, 2, half), F32),
            vmem((2, HD, half), F32),
            vmem((2, 8, half, 2 * HD), BF16),
            vmem((2, half, width), F32),
            vmem((2, width, half), F32),
            vmem((2, width, half), BF16),
            vmem((2, 8, share, half), BF16),
            dma((10,)),
            dma((10,)), dma((10,)), dma((8, 2)), dma((8, 2)),
            dma((8, 2)), dma((7, 2)), dma((8, 2)), dma((7, 2)),
            dma((8,)), dma((8,)), dma((8,)), dma((8,)),
            dma((8, 2)), dma((8, 2)), dma((8, 2)), dma((8, 2)),
        ],
        compiler_params=pltpu.CompilerParams(collective_id=0, has_side_effects=True),
    )(
        tokens[0], stale_k[0], stale_v[0], w_query, w_key, w_value, w_out,
        ff_value, ff_gate, ff_down,
    )
    return result.T[None]


def solution(mesh):
    return jax.shard_map(
        per_device,
        mesh=mesh,
        in_specs=(
            P(None, "patch", None),
            P(None, "patch", "chan"),
            P(None, "patch", "chan"),
            P(None, "chan"),
            P(None, "chan"),
            P(None, "chan"),
            P("chan", None),
            P(None, "chan"),
            P(None, "chan"),
            P("chan", None),
        ),
        out_specs=P(None, "patch", "chan"),
        check_vma=False,
    )
```

```python
import functools
import math

import jax
import jax.numpy as jnp
from jax import lax
from jax.experimental import pallas as pl
from jax.experimental.pallas import tpu as pltpu
from jax.sharding import PartitionSpec as P

HD = 64
MESH = pl.DeviceIdType.MESH
F32 = jnp.float32
BF16 = jnp.bfloat16
LOW = -1e30
SCALE = math.log2(math.e) / math.sqrt(HD)


def normalize(values):
    mean = jnp.mean(values, axis=-1, keepdims=True)
    centered = values - mean
    var = jnp.mean(centered * centered, axis=-1, keepdims=True)
    return centered * lax.rsqrt(var + 1e-05)


def block_kernel(
    tok_hbm, k_hbm, v_hbm, wq_hbm, wk_hbm, wv_hbm, wo_hbm, fv_hbm, fg_hbm, fd_hbm, out,
    tok, k_in, v_in, w_q, w_kv, w_o, f_vg, f_d,
    normed, kvb, kvo, qb, qo, kk, qq, s_a, s_b, b_a, b_b,
    top, total, acc, stat_out, o_out, o_in, stat_in, fin,
    att, resid, turned, down, pieces,
    load, kv_send, kv_recv, q_send, q_recv, o_send, o_recv, t_send, t_recv,
    w_send, w_recv, wx_send, wx_recv, a_send, a_recv, r_send, r_recv,
):
    p, c = lax.axis_index("patch"), lax.axis_index("chan")
    s = lax.rem(p, 2)
    z = lax.rem(lax.div(p, 2), 4)
    y = lax.div(p, 8)
    t = 1 - s
    y_up, y_down = lax.rem(y + 1, 4), lax.rem(y + 3, 4)
    z_up, z_down = lax.rem(z + 1, 4), lax.rem(z + 3, 4)
    y_far, z_far = lax.rem(y + 2, 4), lax.rem(z + 2, 4)
    across, along = lax.div(c, 4), lax.rem(c, 4)
    rows = tok.shape[0]
    half = rows // 2
    share = out.shape[0]
    hidden = f_d.shape[0]

    def dev(y, z, s):
        return ((y * 4 + z) * 2 + s, c)

    partner = dev(y, z, t)

    def chan_of(j):
        return lax.rem(across + j // 4, 2) * 4 + lax.rem(along + j % 4, 4)

    loads = [
        pltpu.make_async_copy(src, dst, load.at[i])
        for i, (src, dst) in enumerate(
            (
                (k_hbm, k_in), (v_hbm, v_in), (tok_hbm, tok), (wq_hbm, w_q),
                (wk_hbm, w_kv.at[:, : 2 * HD]), (wv_hbm, w_kv.at[:, 2 * HD :]), (wo_hbm, w_o.at[0]),
                (fv_hbm, f_vg.at[:, :hidden]), (fg_hbm, f_vg.at[:, hidden:]), (fd_hbm, f_d),
            )
        )
    ]
    for part in loads[:4]:
        part.start()

    barrier = pltpu.get_barrier_semaphore()
    peers = [partner]
    for core in (s, t):
        peers += [dev(y_up, z, core), dev(y_down, z, core)]
        peers += [dev(y, z_up, core), dev(y, z_down, core)]
        peers += [dev(y_far, z, core), dev(y, z_far, core)]
    peers += [(p, chan_of(j)) for j in range(1, 8)]
    for peer in peers:
        pl.semaphore_signal(barrier, inc=1, device_id=peer, device_id_type=MESH)

    def split_heads(values):
        first, second = values[:HD], values[HD:]
        mine = jnp.where(s == 0, first, second)
        other = jnp.where(s == 0, second, first)
        return mine, other

    def copy(src, dst, send, recv, peer):
        return pltpu.make_async_remote_copy(
            src_ref=src, dst_ref=dst, send_sem=send, recv_sem=recv,
            device_id=peer, device_id_type=MESH,
        )

    for j, ref in enumerate((k_in, v_in)):
        loads[j].wait()
        mine, other = split_heads(ref[...].T)
        kvb[0, j] = mine
        kvo[0, j] = other
    pl.semaphore_wait(barrier, len(peers))
    kv = {
        2: copy(kvb.at[0], kvb.at[2], kv_send.at[2], kv_recv.at[2], dev(y_up, z, s)),
        3: copy(kvo.at[0], kvb.at[3], kv_send.at[3], kv_recv.at[3], dev(y_down, z, t)),
        1: copy(kvo.at[0], kvb.at[1], kv_send.at[1], kv_recv.at[1], partner),
        4: copy(kvo.at[0], kvb.at[4], kv_send.at[4], kv_recv.at[4], dev(y_up, z, t)),
        5: copy(kvb.at[0], kvb.at[5], kv_send.at[5], kv_recv.at[5], dev(y_down, z, s)),
        6: copy(kvb.at[0], kvb.at[6], kv_send.at[6], kv_recv.at[6], dev(y_far, z, s)),
        7: copy(kvo.at[0], kvb.at[7], kv_send.at[7], kv_recv.at[7], dev(y_far, z, t)),
        9: copy(kvo.at[1], kvb.at[9], kv_send.at[9], kv_recv.at[9], partner),
    }
    for j in (2, 3, 1, 4, 5, 6, 7):
        kv[j].start()

    mine_rows = pl.ds(pl.multiple_of(s * HD, HD), HD)
    weights = {}
    for j in range(1, 8):
        weights[j] = copy(
            wo_hbm.at[mine_rows] if j < 5 else w_o.at[4, mine_rows],
            w_o.at[j, mine_rows], w_send.at[j], w_recv.at[j],
            (p, chan_of(j if j < 5 else j - 4)),
        )
    passed = {}
    for j in range(1, 8):
        passed[j] = copy(
            w_o.at[j, mine_rows], w_o.at[j, mine_rows], wx_send.at[j], wx_recv.at[j], partner
        )
    for part in loads[4:]:
        part.start()
    for j in (1, 3, 2):
        weights[j].start()

    step = 128
    loads[2].wait()

    def norm_rows(i, _):
        at = pl.ds(pl.multiple_of(i * step, step), step)
        normed[at, :] = normalize(tok[at, :].astype(F32)).astype(BF16)
        return 0

    def project(w, here):
        result = jnp.dot(normed[here], w[...], preferred_element_type=F32)
        return result.astype(BF16).T

    loads[3].wait()
    q = {}
    for h in (0, 1):
        for j, (from_ref, peer) in {
            2: (qb.at[0, h], dev(y, z_up, s)),
            3: (qo.at[h], dev(y, z_down, t)),
            4: (qo.at[h], dev(y, z_up, t)),
            5: (qb.at[0, h], dev(y, z_down, s)),
            1: (qo.at[h], partner),
            6: (qb.at[0, h], dev(y, z_far, s)),
            7: (qo.at[h], dev(y, z_far, t)),
        }.items():
            q[j, h] = copy(from_ref, qb.at[j, h], q_send.at[j, h], q_recv.at[j, h], peer)
    for h in (0, 1):
        lax.fori_loop(h * half // step, (h + 1) * half // step, norm_rows, 0)
        qb[0, h], qo[h] = split_heads(project(w_q, slice(h * half, (h + 1) * half)))
        for j in (1, 2, 3, 4, 5, 6, 7):
            q[j, h].start()
        if h == 0:
            weights[4].start()
    loads[4].wait()
    loads[5].wait()
    both = project(w_kv, slice(0, rows))
    for j in (0, 1):
        kvb[8, j], kvo[1, j] = split_heads(both[j * 2 * HD : (j + 1) * 2 * HD])
    kv[9].start()

    top[...] = jnp.full(top.shape, LOW, F32)
    total[...] = jnp.zeros(total.shape, F32)
    acc[...] = jnp.zeros(acc.shape, F32)

    def prepare_keys(u):
        key = kvb[u, 0]
        kk[u] = jnp.concatenate([key, key], axis=0).T

    def prepare_queries(f, h):
        scaled = qb[f, h].astype(F32) * SCALE
        high = scaled.astype(BF16)
        low = (scaled - high.astype(F32)).astype(BF16)
        qq[f, h] = jnp.concatenate([high, low], axis=0)

    def score(item, s_ref, b_ref):
        h, pair, *units = item
        for side, u in enumerate(units):
            values = jnp.dot(kk[u], qq[2 * pair + side, h], preferred_element_type=F32)
            s_ref[side] = values
            b_ref[side] = jnp.max(values, axis=0, keepdims=True)

    def absorb(item, s_ref, b_ref):
        h, pair, *units = item
        for side, u in enumerate(units):
            f = 2 * pair + side
            old = top[f, h]
            new = jnp.maximum(old, b_ref[side])
            rescale = jnp.exp2(old - new)
            weights = jnp.exp2(s_ref[side] - new)
            total[f, h] = total[f, h] * rescale + jnp.sum(weights, axis=0, keepdims=True)
            acc[f, h] = acc[f, h] * rescale + jnp.dot(
                kvb[u, 1], weights.astype(BF16), preferred_element_type=F32
            )
            top[f, h] = new

    def block(h, first_pair, pairs, first_unit, units):
        def item(i):
            i = jnp.int32(i)
            u = first_unit + lax.rem(i, units)
            return jnp.int32(h), first_pair + lax.div(i, units), u, u

        return pairs * units, item

    def own_block(h):
        def item(i):
            i = jnp.int32(i)
            return jnp.int32(h), jnp.int32(0), 8 - 7 * i, 9 * i

        return 2, item

    def attend(this, then=None, started=False):
        count, item = this
        if not started:
            score(item(0), s_a, b_a)
        following = item(count - 1) if then is None else then[1](0)

        def two(i, _):
            first, second = item(2 * i), item(2 * i + 1)
            more = 2 * i + 2 < count
            third = tuple(
                jnp.where(more, inner, after)
                for inner, after in zip(item(2 * i + 2), following)
            )
            score(second, s_b, b_b)
            absorb(first, s_a, b_a)
            score(third, s_a, b_a)
            absorb(second, s_b, b_b)
            return 0

        lax.fori_loop(0, count // 2, two, 0)

    def keys_ready(*units):
        for u in units:
            kv[u].wait_recv()
            prepare_keys(u)

    def queries_ready(h, *units):
        for f in units:
            q[f, h].wait_recv()
            prepare_queries(f, h)

    targets = {
        6: (dev(y, z_far, s), 5),
        7: (dev(y, z_far, t), 6),
        2: (dev(y, z_down, s), 1),
        3: (dev(y, z_up, t), 2),
        4: (dev(y, z_down, t), 3),
        5: (dev(y, z_up, s), 4),
        1: (partner, 0),
    }
    back = {}
    for h in (0, 1):
        for f, (peer, slot) in targets.items():
            back[f, h] = (
                copy(
                    o_out.at[f, h], o_in.at[slot, h], o_send.at[f, h], o_recv.at[slot, h], peer
                ),
                copy(
                    stat_out.at[f, h], stat_in.at[slot, h], t_send.at[f, h],
                    t_recv.at[slot, h], peer,
                ),
            )

    def give(h, *units):
        for f in units:
            o_out[f, h] = acc[f, h].astype(BF16)
            stat_out[f, h, 0:1] = top[f, h]
            stat_out[f, h, 1:2] = total[f, h]
            for part in back[f, h]:
                part.start()

    def arrived(h, *units):
        for f in units:
            for part in back[f, h]:
                part.wait_recv()

    def merge(one, other):
        new = jnp.maximum(one[0], other[0])
        left, right = jnp.exp2(one[0] - new), jnp.exp2(other[0] - new)
        return (
            new,
            one[1] * left + other[1] * right,
            one[2] * left + other[2] * right,
        )

    def received(h, slot):
        return stat_in[slot, h, 0:1], stat_in[slot, h, 1:2], o_in[slot, h].astype(F32)

    def local(h, f):
        return top[f, h], total[f, h], acc[f, h]

    gathers = {}
    for h in (0, 1):
        for j in range(1, 8):
            relay = h == 0 and j > 4
            gathers[j, h] = copy(
                att.at[h, 4 if relay else 0], att.at[h, j], a_send.at[j, h], a_recv.at[j, h],
                (p, chan_of(j - 4 if relay else j)),
            )

    def finish(h):
        arrived(h, 1, 2, 3, 4, 5, 6, 7)
        for head, parts in (
            (s, (local(h, 0), received(h, 1), received(h, 4), received(h, 5))),
            (t, (received(h, 0), received(h, 2), received(h, 3), received(h, 6))),
        ):
            _, sums, values = functools.reduce(merge, parts)
            fin[head] = values / sums
        att[h, 0] = jnp.concatenate([fin[0], fin[1]], axis=0).T.astype(BF16)
        for j in (4, 1, 3, 2) if h == 0 else (1, 3, 4, 2, 5, 7, 6):
            gathers[j, h].start()

    scatters = {}
    for h in (0, 1):
        for j in range(1, 8):
            chunk = pl.ds(pl.multiple_of(chan_of(j) * share, 32), share)
            scatters[j, h] = copy(
                down.at[h, chunk], pieces.at[h, j], r_send.at[j, h], r_recv.at[j, h],
                (p, chan_of(j)),
            )
    my_chunk = pl.ds(pl.multiple_of(c * share, 32), share)

    def feed_forward(h):
        here = slice(h * half, (h + 1) * half)
        mixed = tok[here].astype(F32)
        for j in range(0, 8, 2):
            for arriving in (j, j + 1):
                if arriving != 0 and (h == 1 or arriving != 4):
                    gathers[arriving, h].wait_recv()
            mixed += jnp.dot(
                jnp.concatenate([att[h, j], att[h, j + 1]], axis=1),
                w_o[j : j + 2].reshape(4 * HD, w_o.shape[2]),
                preferred_element_type=F32,
            )
        resid[h] = mixed

        def norm_again(i, _):
            at = pl.ds(pl.multiple_of(i * step, step), step)
            normed[at, :] = normalize(resid[h, at, :]).astype(BF16)
            return 0

        lax.fori_loop(0, half // step, norm_again, 0)
        inputs = normed[:half]
        both = jnp.dot(inputs, f_vg[...], preferred_element_type=F32)
        values, gate = both[:, :hidden], both[:, hidden:]
        gate = 0.5 * gate * (1.0 + lax.erf(gate * math.sqrt(0.5)))
        gated = (values * gate).astype(BF16)
        result = jnp.dot(gated, f_d[...], preferred_element_type=F32)
        down[h] = result.astype(BF16).T
        for j in (5, 7, 4, 1, 3, 6, 2):
            scatters[j, h].start()

    def conclude(h):
        turned[h] = resid[h].T
        sums = turned[h, my_chunk] + down[h, my_chunk].astype(F32)
        for j in range(1, 8):
            scatters[j, h].wait_recv()
            sums += pieces[h, j].astype(F32)
        out[:, h * half : (h + 1) * half] = sums.astype(out.dtype)

    prepare_keys(0)
    prepare_keys(8)
    prepare_queries(0, 0)
    prepare_queries(0, 1)
    keys_ready(1, 9)
    queries_ready(0, 1)
    queries_ready(1, 1)
    attend(own_block(0), own_block(1))
    attend(own_block(1), started=True)
    keys_ready(2, 3)
    attend(block(0, 0, 1, 2, 2), block(1, 0, 1, 2, 2))
    attend(block(1, 0, 1, 2, 2), started=True)
    queries_ready(0, 2, 3)
    attend(block(0, 1, 1, 0, 4))
    keys_ready(4, 5)
    queries_ready(0, 4, 5)
    attend(block(0, 1, 1, 4, 2), block(0, 2, 1, 0, 6))
    attend(block(0, 2, 1, 0, 6), block(0, 0, 1, 4, 2), started=True)
    attend(block(0, 0, 1, 4, 2), started=True)
    queries_ready(0, 6, 7)
    keys_ready(6, 7)
    ahead = [
        block(0, 1, 1, 6, 2), block(0, 2, 1, 6, 2), block(0, 3, 1, 0, 8), block(0, 0, 1, 6, 2),
        block(1, 3, 1, 0, 8), block(1, 1, 1, 0, 8), block(1, 2, 1, 0, 8), block(1, 0, 1, 4, 4),
    ]
    attend(ahead[0], ahead[1])
    give(0, 2, 3)
    attend(ahead[1], ahead[2], started=True)
    give(0, 4, 5)
    attend(ahead[2], ahead[3], started=True)
    give(0, 6, 7)
    attend(ahead[3], started=True)
    give(0, 1)
    weights[4].wait_recv()
    for j in (5, 7, 6):
        weights[j].start()
    queries_ready(1, 2, 3, 4, 5, 6, 7)
    attend(ahead[4], ahead[5])
    give(1, 6, 7)
    for j in (1, 2, 3):
        weights[j].wait_recv()
    for j in (1, 2, 3, 4):
        passed[j].start()
    attend(ahead[5], ahead[6], started=True)
    give(1, 2, 3)
    finish(0)
    attend(ahead[6], ahead[7], started=True)
    give(1, 4, 5)
    attend(ahead[7], started=True)
    give(1, 1)
    gathers[4, 0].wait_recv()
    for j in (5, 7, 6):
        gathers[j, 0].start()
    for j in (5, 7, 6):
        weights[j].wait_recv()
        passed[j].start()
    finish(1)
    for part in loads[6:]:
        part.wait()
    for j in range(1, 8):
        passed[j].wait_recv()
    feed_forward(0)
    feed_forward(1)
    conclude(0)
    conclude(1)

    for j in (1, 2, 3, 4, 5, 6, 7, 9):
        kv[j].wait_send()
    for j in range(1, 8):
        weights[j].wait_send()
        passed[j].wait_send()
        for h in (0, 1):
            q[j, h].wait_send()
            for part in back[j, h]:
                part.wait_send()
            gathers[j, h].wait_send()
            scatters[j, h].wait_send()


def per_device(
    tokens, stale_k, stale_v, w_query, w_key, w_value, w_out, ff_value, ff_gate, ff_down
):
    _, rows, width = tokens.shape
    half, hidden = rows // 2, ff_value.shape[1]
    share = width // lax.axis_size("chan")
    vmem, dma = pltpu.VMEM, pltpu.SemaphoreType.DMA
    result = pl.pallas_call(
        block_kernel,
        out_shape=jax.ShapeDtypeStruct((share, rows), BF16),
        in_specs=[pl.BlockSpec(memory_space=pl.ANY)] * 10,
        out_specs=pl.BlockSpec(memory_space=vmem),
        scratch_shapes=[
            vmem((rows, width), BF16),
            vmem((rows, 2 * HD), BF16),
            vmem((rows, 2 * HD), BF16),
            vmem((width, 2 * HD), BF16),
            vmem((width, 4 * HD), BF16),
            vmem((8, 2 * HD, width), BF16),
            vmem((width, 2 * hidden), BF16),
            vmem((hidden, width), BF16),
            vmem((rows, width), BF16),
            vmem((10, 2, HD, rows), BF16),
            vmem((2, 2, HD, rows), BF16),
            vmem((8, 2, HD, half), BF16),
            vmem((2, HD, half), BF16),
            vmem((10, rows, 2 * HD), BF16),
            vmem((8, 2, 2 * HD, half), BF16),
            vmem((2, rows, half), F32),
            vmem((2, rows, half), F32),
            vmem((2, 1, half), F32),
            vmem((2, 1, half), F32),
            vmem((8, 2, 1, half), F32),
            vmem((8, 2, 1, half), F32),
            vmem((8, 2, HD, half), F32),
            vmem((8, 2, 2, half), F32),
            vmem((8, 2, HD, half), BF16),
            vmem((7, 2, HD, half), BF16),
            vmem((7, 2, 2, half), F32),
            vmem((2, HD, half), F32),
            vmem((2, 8, half, 2 * HD), BF16),
            vmem((2, half, width), F32),
            vmem((2, width, half), F32),
            vmem((2, width, half), BF16),
            vmem((2, 8, share, half), BF16),
            dma((10,)),
            dma((10,)), dma((10,)), dma((8, 2)), dma((8, 2)),
            dma((8, 2)), dma((7, 2)), dma((8, 2)), dma((7, 2)),
            dma((8,)), dma((8,)), dma((8,)), dma((8,)),
            dma((8, 2)), dma((8, 2)), dma((8, 2)), dma((8, 2)),
        ],
        compiler_params=pltpu.CompilerParams(
            collective_id=0,
            has_side_effects=True,
        ),
    )(
        tokens[0], stale_k[0], stale_v[0], w_query, w_key, w_value, w_out,
        ff_value, ff_gate, ff_down,
    )
    return result.T[None]


def solution(mesh):
    return jax.shard_map(
        per_device,
        mesh=mesh,
        in_specs=(
            P(None, "patch", None),
            P(None, "patch", "chan"),
            P(None, "patch", "chan"),
            P(None, "chan"),
            P(None, "chan"),
            P(None, "chan"),
            P("chan", None),
            P(None, "chan"),
            P(None, "chan"),
            P("chan", None),
        ),
        out_specs=P(None, "patch", "chan"),
        check_vma=False,
    )
```

```python
import functools
import math

import jax
import jax.numpy as jnp
from jax import lax
from jax.experimental import pallas as pl
from jax.experimental.pallas import tpu as pltpu
from jax.sharding import PartitionSpec as P

HD = 64
MESH = pl.DeviceIdType.MESH
F32 = jnp.float32
BF16 = jnp.bfloat16
LOW = -1e30
SCALE = math.log2(math.e) / math.sqrt(HD)


def normalize(values):
    mean = jnp.mean(values, axis=-1, keepdims=True)
    centered = values - mean
    var = jnp.mean(centered * centered, axis=-1, keepdims=True)
    return centered * lax.rsqrt(var + 1e-05)


def block_kernel(
    tok_hbm, k_hbm, v_hbm, wq_hbm, wk_hbm, wv_hbm, wo_hbm, fv_hbm, fg_hbm, fd_hbm, out,
    tok, k_in, v_in, w_q, w_kv, w_o, f_vg, f_d,
    normed, kvb, kvo, qb, qo, kk, qq, s_a, s_b, b_a, b_b,
    top, total, acc, stat_out, o_out, o_in, stat_in, fin,
    att, resid, turned, down, pieces,
    load, kv_send, kv_recv, q_send, q_recv, o_send, o_recv, t_send, t_recv,
    w_send, w_recv, wx_send, wx_recv, a_send, a_recv, r_send, r_recv,
):
    p, c = lax.axis_index("patch"), lax.axis_index("chan")
    s = lax.rem(p, 2)
    z = lax.rem(lax.div(p, 2), 4)
    y = lax.div(p, 8)
    t = 1 - s
    y_up, y_down = lax.rem(y + 1, 4), lax.rem(y + 3, 4)
    z_up, z_down = lax.rem(z + 1, 4), lax.rem(z + 3, 4)
    y_far, z_far = lax.rem(y + 2, 4), lax.rem(z + 2, 4)
    across, along = lax.div(c, 4), lax.rem(c, 4)
    rows = tok.shape[0]
    half = rows // 2
    share = out.shape[0]
    hidden = f_d.shape[0]

    def dev(y, z, s):
        return ((y * 4 + z) * 2 + s, c)

    partner = dev(y, z, t)

    def chan_of(j):
        return lax.rem(across + j // 4, 2) * 4 + lax.rem(along + j % 4, 4)

    loads = [
        pltpu.make_async_copy(src, dst, load.at[i])
        for i, (src, dst) in enumerate(
            (
                (k_hbm, k_in), (v_hbm, v_in), (tok_hbm, tok), (wq_hbm, w_q),
                (wk_hbm, w_kv.at[:, : 2 * HD]), (wv_hbm, w_kv.at[:, 2 * HD :]), (wo_hbm, w_o.at[0]),
                (fv_hbm, f_vg.at[:, :hidden]), (fg_hbm, f_vg.at[:, hidden:]), (fd_hbm, f_d),
            )
        )
    ]
    for part in loads[:4]:
        part.start()

    barrier = pltpu.get_barrier_semaphore()
    peers = [partner]
    for core in (s, t):
        peers += [dev(y_up, z, core), dev(y_down, z, core)]
        peers += [dev(y, z_up, core), dev(y, z_down, core)]
        peers += [dev(y_far, z, core), dev(y, z_far, core)]
    peers += [(p, chan_of(j)) for j in range(1, 8)]
    for peer in peers:
        pl.semaphore_signal(barrier, inc=1, device_id=peer, device_id_type=MESH)

    def split_heads(values):
        first, second = values[:HD], values[HD:]
        mine = jnp.where(s == 0, first, second)
        other = jnp.where(s == 0, second, first)
        return mine, other

    def copy(src, dst, send, recv, peer):
        return pltpu.make_async_remote_copy(
            src_ref=src, dst_ref=dst, send_sem=send, recv_sem=recv,
            device_id=peer, device_id_type=MESH,
        )

    for j, ref in enumerate((k_in, v_in)):
        loads[j].wait()
        mine, other = split_heads(ref[...].T)
        kvb[0, j] = mine
        kvo[0, j] = other
    pl.semaphore_wait(barrier, len(peers))
    kv = {
        2: copy(kvb.at[0], kvb.at[2], kv_send.at[2], kv_recv.at[2], dev(y_up, z, s)),
        3: copy(kvo.at[0], kvb.at[3], kv_send.at[3], kv_recv.at[3], dev(y_down, z, t)),
        1: copy(kvo.at[0], kvb.at[1], kv_send.at[1], kv_recv.at[1], partner),
        4: copy(kvo.at[0], kvb.at[4], kv_send.at[4], kv_recv.at[4], dev(y_up, z, t)),
        5: copy(kvb.at[0], kvb.at[5], kv_send.at[5], kv_recv.at[5], dev(y_down, z, s)),
        6: copy(kvb.at[0], kvb.at[6], kv_send.at[6], kv_recv.at[6], dev(y_far, z, s)),
        7: copy(kvo.at[0], kvb.at[7], kv_send.at[7], kv_recv.at[7], dev(y_far, z, t)),
        9: copy(kvo.at[1], kvb.at[9], kv_send.at[9], kv_recv.at[9], partner),
    }
    for j in (2, 3, 1, 4, 5, 6, 7):
        kv[j].start()

    mine_rows = pl.ds(pl.multiple_of(s * HD, HD), HD)
    weights = {}
    for j in range(1, 8):
        weights[j] = copy(
            wo_hbm.at[mine_rows] if j < 5 else w_o.at[4, mine_rows],
            w_o.at[j, mine_rows], w_send.at[j], w_recv.at[j],
            (p, chan_of(j if j < 5 else j - 4)),
        )
    passed = {}
    for j in range(1, 8):
        passed[j] = copy(
            w_o.at[j, mine_rows], w_o.at[j, mine_rows], wx_send.at[j], wx_recv.at[j], partner
        )
    for part in loads[4:]:
        part.start()
    for j in (1, 3, 2):
        weights[j].start()

    step = 128
    loads[2].wait()

    def norm_rows(i, _):
        at = pl.ds(pl.multiple_of(i * step, step), step)
        normed[at, :] = normalize(tok[at, :].astype(F32)).astype(BF16)
        return 0

    def project(w, here):
        result = jnp.dot(normed[here], w[...], preferred_element_type=F32)
        return result.astype(BF16).T

    loads[3].wait()
    q = {}
    for h in (0, 1):
        for j, (from_ref, peer) in {
            2: (qb.at[0, h], dev(y, z_up, s)),
            3: (qo.at[h], dev(y, z_down, t)),
            4: (qo.at[h], dev(y, z_up, t)),
            5: (qb.at[0, h], dev(y, z_down, s)),
            1: (qo.at[h], partner),
            6: (qb.at[0, h], dev(y, z_far, s)),
            7: (qo.at[h], dev(y, z_far, t)),
        }.items():
            q[j, h] = copy(from_ref, qb.at[j, h], q_send.at[j, h], q_recv.at[j, h], peer)
    for h in (0, 1):
        lax.fori_loop(h * half // step, (h + 1) * half // step, norm_rows, 0)
        qb[0, h], qo[h] = split_heads(project(w_q, slice(h * half, (h + 1) * half)))
        for j in (1, 2, 3, 4, 5, 6, 7):
            q[j, h].start()
        if h == 0:
            weights[4].start()
    loads[4].wait()
    loads[5].wait()
    both = project(w_kv, slice(0, rows))
    for j in (0, 1):
        kvb[8, j], kvo[1, j] = split_heads(both[j * 2 * HD : (j + 1) * 2 * HD])
    kv[9].start()

    top[...] = jnp.full(top.shape, LOW, F32)
    total[...] = jnp.zeros(total.shape, F32)
    acc[...] = jnp.zeros(acc.shape, F32)

    def prepare_keys(u):
        key = kvb[u, 0]
        kk[u] = jnp.concatenate([key, key], axis=0).T

    def prepare_queries(f, h):
        scaled = qb[f, h].astype(F32) * SCALE
        high = scaled.astype(BF16)
        low = (scaled - high.astype(F32)).astype(BF16)
        qq[f, h] = jnp.concatenate([high, low], axis=0)

    def score(item, s_ref, b_ref):
        h, pair, *units = item
        for side, u in enumerate(units):
            values = jnp.dot(kk[u], qq[2 * pair + side, h], preferred_element_type=F32)
            s_ref[side] = values
            b_ref[side] = jnp.max(values, axis=0, keepdims=True)

    def absorb(item, s_ref, b_ref):
        h, pair, *units = item
        for side, u in enumerate(units):
            f = 2 * pair + side
            old = top[f, h]
            new = jnp.maximum(old, b_ref[side])
            rescale = jnp.exp2(old - new)
            weights = jnp.exp2(s_ref[side] - new)
            total[f, h] = total[f, h] * rescale + jnp.sum(weights, axis=0, keepdims=True)
            acc[f, h] = acc[f, h] * rescale + jnp.dot(
                kvb[u, 1], weights.astype(BF16), preferred_element_type=F32
            )
            top[f, h] = new

    def block(h, first_pair, pairs, first_unit, units):
        def item(i):
            i = jnp.int32(i)
            u = first_unit + lax.rem(i, units)
            return jnp.int32(h), first_pair + lax.div(i, units), u, u

        return pairs * units, item

    def own_block(h):
        def item(i):
            i = jnp.int32(i)
            return jnp.int32(h), jnp.int32(0), 8 - 7 * i, 9 * i

        return 2, item

    def attend(this, then=None, started=False):
        count, item = this
        if not started:
            score(item(0), s_a, b_a)
        following = item(count - 1) if then is None else then[1](0)

        def two(i, _):
            first, second = item(2 * i), item(2 * i + 1)
            more = 2 * i + 2 < count
            third = tuple(
                jnp.where(more, inner, after)
                for inner, after in zip(item(2 * i + 2), following)
            )
            score(second, s_b, b_b)
            absorb(first, s_a, b_a)
            score(third, s_a, b_a)
            absorb(second, s_b, b_b)
            return 0

        lax.fori_loop(0, count // 2, two, 0)

    def keys_ready(*units):
        for u in units:
            kv[u].wait_recv()
            prepare_keys(u)

    def queries_ready(h, *units):
        for f in units:
            q[f, h].wait_recv()
            prepare_queries(f, h)

    targets = {
        6: (dev(y, z_far, s), 5),
        7: (dev(y, z_far, t), 6),
        2: (dev(y, z_down, s), 1),
        3: (dev(y, z_up, t), 2),
        4: (dev(y, z_down, t), 3),
        5: (dev(y, z_up, s), 4),
        1: (partner, 0),
    }
    back = {}
    for h in (0, 1):
        for f, (peer, slot) in targets.items():
            back[f, h] = (
                copy(
                    o_out.at[f, h], o_in.at[slot, h], o_send.at[f, h], o_recv.at[slot, h], peer
                ),
                copy(
                    stat_out.at[f, h], stat_in.at[slot, h], t_send.at[f, h],
                    t_recv.at[slot, h], peer,
                ),
            )

    def give(h, *units):
        for f in units:
            o_out[f, h] = acc[f, h].astype(BF16)
            stat_out[f, h, 0:1] = top[f, h]
            stat_out[f, h, 1:2] = total[f, h]
            for part in back[f, h]:
                part.start()

    def arrived(h, *units):
        for f in units:
            for part in back[f, h]:
                part.wait_recv()

    def merge(one, other):
        new = jnp.maximum(one[0], other[0])
        left, right = jnp.exp2(one[0] - new), jnp.exp2(other[0] - new)
        return (
            new,
            one[1] * left + other[1] * right,
            one[2] * left + other[2] * right,
        )

    def received(h, slot):
        return stat_in[slot, h, 0:1], stat_in[slot, h, 1:2], o_in[slot, h].astype(F32)

    def local(h, f):
        return top[f, h], total[f, h], acc[f, h]

    gathers = {}
    for h in (0, 1):
        for j in range(1, 8):
            relay = h == 0 and j > 4
            gathers[j, h] = copy(
                att.at[h, 4 if relay else 0], att.at[h, j], a_send.at[j, h], a_recv.at[j, h],
                (p, chan_of(j - 4 if relay else j)),
            )

    def finish(h):
        arrived(h, 1, 2, 3, 4, 5, 6, 7)
        for head, parts in (
            (s, (local(h, 0), received(h, 1), received(h, 4), received(h, 5))),
            (t, (received(h, 0), received(h, 2), received(h, 3), received(h, 6))),
        ):
            _, sums, values = functools.reduce(merge, parts)
            fin[head] = values / sums
        att[h, 0] = jnp.concatenate([fin[0], fin[1]], axis=0).T.astype(BF16)
        for j in (4, 1, 3, 2) if h == 0 else (1, 3, 4, 2, 5, 7, 6):
            gathers[j, h].start()

    scatters = {}
    for h in (0, 1):
        for j in range(1, 8):
            chunk = pl.ds(pl.multiple_of(chan_of(j) * share, 32), share)
            scatters[j, h] = copy(
                down.at[h, chunk], pieces.at[h, j], r_send.at[j, h], r_recv.at[j, h],
                (p, chan_of(j)),
            )
    my_chunk = pl.ds(pl.multiple_of(c * share, 32), share)

    def feed_forward(h):
        here = slice(h * half, (h + 1) * half)
        mixed = tok[here].astype(F32)
        for j in range(0, 8, 2):
            for arriving in (j, j + 1):
                if arriving != 0 and (h == 1 or arriving != 4):
                    gathers[arriving, h].wait_recv()
            mixed += jnp.dot(
                jnp.concatenate([att[h, j], att[h, j + 1]], axis=1),
                w_o[j : j + 2].reshape(4 * HD, w_o.shape[2]),
                preferred_element_type=F32,
            )
        resid[h] = mixed

        def norm_again(i, _):
            at = pl.ds(pl.multiple_of(i * step, step), step)
            normed[at, :] = normalize(resid[h, at, :]).astype(BF16)
            return 0

        lax.fori_loop(0, half // step, norm_again, 0)
        inputs = normed[:half]
        both = jnp.dot(inputs, f_vg[...], preferred_element_type=F32)
        values, gate = both[:, :hidden], both[:, hidden:]
        gate = 0.5 * gate * (1.0 + lax.erf(gate * math.sqrt(0.5)))
        gated = (values * gate).astype(BF16)
        result = jnp.dot(gated, f_d[...], preferred_element_type=F32)
        down[h] = result.astype(BF16).T
        for j in (5, 7, 4, 1, 3, 6, 2):
            scatters[j, h].start()

    def conclude(h):
        turned[h] = resid[h].T
        sums = turned[h, my_chunk] + down[h, my_chunk].astype(F32)
        for j in range(1, 8):
            scatters[j, h].wait_recv()
            sums += pieces[h, j].astype(F32)
        out[:, h * half : (h + 1) * half] = sums

    prepare_keys(0)
    prepare_keys(8)
    prepare_queries(0, 0)
    prepare_queries(0, 1)
    keys_ready(1, 9)
    queries_ready(0, 1)
    queries_ready(1, 1)
    attend(own_block(0), own_block(1))
    attend(own_block(1), started=True)
    keys_ready(2, 3)
    attend(block(0, 0, 1, 2, 2), block(1, 0, 1, 2, 2))
    attend(block(1, 0, 1, 2, 2), started=True)
    queries_ready(0, 2, 3)
    attend(block(0, 1, 1, 0, 4))
    keys_ready(4, 5)
    queries_ready(0, 4, 5)
    attend(block(0, 1, 1, 4, 2), block(0, 2, 1, 0, 6))
    attend(block(0, 2, 1, 0, 6), block(0, 0, 1, 4, 2), started=True)
    attend(block(0, 0, 1, 4, 2), started=True)
    queries_ready(0, 6, 7)
    keys_ready(6, 7)
    ahead = [
        block(0, 1, 1, 6, 2), block(0, 2, 1, 6, 2), block(0, 3, 1, 0, 8), block(0, 0, 1, 6, 2),
        block(1, 3, 1, 0, 8), block(1, 1, 1, 0, 8), block(1, 2, 1, 0, 8), block(1, 0, 1, 4, 4),
    ]
    attend(ahead[0], ahead[1])
    give(0, 2, 3)
    attend(ahead[1], ahead[2], started=True)
    give(0, 4, 5)
    attend(ahead[2], ahead[3], started=True)
    give(0, 6, 7)
    attend(ahead[3], started=True)
    give(0, 1)
    weights[4].wait_recv()
    for j in (5, 7, 6):
        weights[j].start()
    queries_ready(1, 2, 3, 4, 5, 6, 7)
    attend(ahead[4], ahead[5])
    give(1, 6, 7)
    for j in (1, 2, 3):
        weights[j].wait_recv()
    for j in (1, 2, 3, 4):
        passed[j].start()
    attend(ahead[5], ahead[6], started=True)
    give(1, 2, 3)
    finish(0)
    attend(ahead[6], ahead[7], started=True)
    give(1, 4, 5)
    attend(ahead[7], started=True)
    give(1, 1)
    gathers[4, 0].wait_recv()
    for j in (5, 7, 6):
        gathers[j, 0].start()
    for j in (5, 7, 6):
        weights[j].wait_recv()
        passed[j].start()
    finish(1)
    for part in loads[6:]:
        part.wait()
    for j in range(1, 8):
        passed[j].wait_recv()
    feed_forward(0)
    feed_forward(1)
    conclude(0)
    conclude(1)

    for j in (1, 2, 3, 4, 5, 6, 7, 9):
        kv[j].wait_send()
    for j in range(1, 8):
        weights[j].wait_send()
        passed[j].wait_send()
        for h in (0, 1):
            q[j, h].wait_send()
            for part in back[j, h]:
                part.wait_send()
            gathers[j, h].wait_send()
            scatters[j, h].wait_send()


def per_device(
    tokens, stale_k, stale_v, w_query, w_key, w_value, w_out, ff_value, ff_gate, ff_down
):
    _, rows, width = tokens.shape
    half, hidden = rows // 2, ff_value.shape[1]
    share = width // lax.axis_size("chan")
    vmem, dma = pltpu.VMEM, pltpu.SemaphoreType.DMA
    result = pl.pallas_call(
        block_kernel,
        out_shape=jax.ShapeDtypeStruct((share, rows), F32),
        in_specs=[pl.BlockSpec(memory_space=pl.ANY)] * 10,
        out_specs=pl.BlockSpec(memory_space=vmem),
        scratch_shapes=[
            vmem((rows, width), BF16),
            vmem((rows, 2 * HD), BF16),
            vmem((rows, 2 * HD), BF16),
            vmem((width, 2 * HD), BF16),
            vmem((width, 4 * HD), BF16),
            vmem((8, 2 * HD, width), BF16),
            vmem((width, 2 * hidden), BF16),
            vmem((hidden, width), BF16),
            vmem((rows, width), BF16),
            vmem((10, 2, HD, rows), BF16),
            vmem((2, 2, HD, rows), BF16),
            vmem((8, 2, HD, half), BF16),
            vmem((2, HD, half), BF16),
            vmem((10, rows, 2 * HD), BF16),
            vmem((8, 2, 2 * HD, half), BF16),
            vmem((2, rows, half), F32),
            vmem((2, rows, half), F32),
            vmem((2, 1, half), F32),
            vmem((2, 1, half), F32),
            vmem((8, 2, 1, half), F32),
            vmem((8, 2, 1, half), F32),
            vmem((8, 2, HD, half), F32),
            vmem((8, 2, 2, half), F32),
            vmem((8, 2, HD, half), BF16),
            vmem((7, 2, HD, half), BF16),
            vmem((7, 2, 2, half), F32),
            vmem((2, HD, half), F32),
            vmem((2, 8, half, 2 * HD), BF16),
            vmem((2, half, width), F32),
            vmem((2, width, half), F32),
            vmem((2, width, half), BF16),
            vmem((2, 8, share, half), BF16),
            dma((10,)),
            dma((10,)), dma((10,)), dma((8, 2)), dma((8, 2)),
            dma((8, 2)), dma((7, 2)), dma((8, 2)), dma((7, 2)),
            dma((8,)), dma((8,)), dma((8,)), dma((8,)),
            dma((8, 2)), dma((8, 2)), dma((8, 2)), dma((8, 2)),
        ],
        compiler_params=pltpu.CompilerParams(
            collective_id=0,
            has_side_effects=True,
        ),
    )(
        tokens[0], stale_k[0], stale_v[0], w_query, w_key, w_value, w_out,
        ff_value, ff_gate, ff_down,
    )
    return result.T.astype(BF16)[None]


def solution(mesh):
    return jax.shard_map(
        per_device,
        mesh=mesh,
        in_specs=(
            P(None, "patch", None),
            P(None, "patch", "chan"),
            P(None, "patch", "chan"),
            P(None, "chan"),
            P(None, "chan"),
            P(None, "chan"),
            P("chan", None),
            P(None, "chan"),
            P(None, "chan"),
            P("chan", None),
        ),
        out_specs=P(None, "patch", "chan"),
        check_vma=False,
    )
```
